32 devices in a mesh: mission: 2 (over x), arc: 16 (over z, y, core).
Axes of the slice: x: 2, y: 2, z: 4, core: 2. Of those that a mesh axis runs over, the one named last changes fastest.
Arguments:
- design: bfloat16 [2560, 5120], P(('mission', 'arc')), may hold values from -3 to 3
- nuisance_design: bfloat16 [2560, 128], P(('mission', 'arc')), may hold values from -1 to 1
- observed: float32 [2560], P(('mission', 'arc')), may hold values from -6 to 6
- arc_of_row: int32 [2560], P(('mission', 'arc')), may hold values from 0 to 1, as said below
- nuis_size: int32 [64], P(('mission', 'arc')), may hold values from 32 to 128
- weight_index: int32 [2560], P(('mission', 'arc')), may hold values from 0 to 7
- kind_weight: float32 [8], replicated, may hold values from 0.3 to 3
- mission_weight: float32 [2], P('mission'), may hold values from 0.3 to 3
Outputs:
- normal_fold: float32 [2560, 5120], P(('mission', 'arc'))
- right_side: float32 [5120], P(('mission', 'arc'))
- tail_diagonal: float32 [2560], P(('mission', 'arc'))
The draws below stay inside these ranges and needn't reach their ends.
Inputs may be any that keep to these rules, and one draw needn't show every extreme that they name: `arc_of_row`: in each row block of 80 rows the rows of arc 0 come first and those of arc 1 follow; each arc has at least 20 rows.
All inputs are finite; a program needn't handle non-finite values.
Results may differ from the reference program's by a relative error of at most 0.019.
Values may be sent and summed in bfloat16 or wider, within the bound.
A program may use at most 192 MiB of HBM per device.

```python
import math
import jax
import jax.numpy as jnp
from jax import lax

P_SIZE = 5120
NUIS = 128
KINDS = 8
ARCS_DEV = 2
OBS_DEV = 80
HALF = 2560
OBS = 2560
ARCS = 64
N_MISSION = 2
N_ARC = 16


def draw_design(key, part):
    noise_key = jax.random.fold_in(jax.random.fold_in(key, 11), 0)
    freq_key = jax.random.fold_in(jax.random.fold_in(key, 11), 1)
    phase_key = jax.random.fold_in(jax.random.fold_in(key, 11), 2)
    perm_key = jax.random.fold_in(jax.random.fold_in(key, 11), 4)
    columns = jnp.arange(P_SIZE, dtype=jnp.float32)
    noise_part = jnp.clip(jax.random.normal(noise_key, (OBS, P_SIZE), jnp.float32), -6.0, 6.0)
    mode_count = 4
    frequency = jnp.exp(jax.random.uniform(freq_key, (OBS, mode_count), jnp.float32, math.log(0.001), 0.0))
    phases = jax.random.uniform(phase_key, (OBS, mode_count), jnp.float32, -math.pi, math.pi)
    smooth = jnp.zeros((OBS, P_SIZE), jnp.float32)
    for mode_id in range(mode_count):
        smooth = smooth + jnp.cos(frequency[:, mode_id:mode_id + 1] * columns[None, :] + phases[:, mode_id:mode_id + 1])
    values = noise_part + math.sqrt(2.0 / mode_count) * smooth
    blocks = OBS // OBS_DEV
    block_width = P_SIZE // blocks
    target = jax.random.permutation(perm_key, blocks)
    row_block = jnp.arange(OBS, dtype=jnp.int32) // OBS_DEV
    col_block = jnp.arange(P_SIZE, dtype=jnp.int32) // block_width
    spike_gain = jnp.where(target[row_block][:, None] == col_block[None, :], 6.0, 1.0)
    scaled = values * spike_gain / math.sqrt(OBS)
    return jnp.clip(scaled, -3.0, 3.0).astype(jnp.bfloat16)


def draw_arc_of_row(key, part):
    blocks = OBS // OBS_DEV
    split_at = jax.random.randint(jax.random.fold_in(key, 23), (blocks, 1), OBS_DEV // 4, 3 * OBS_DEV // 4 + 1)
    position = jnp.arange(OBS_DEV, dtype=jnp.int32)[None, :]
    return (position >= split_at).astype(jnp.int32).reshape(OBS)


def touch_ends(values, rng, least, top_value):
    shape = values.shape
    index_at = [jax.random.randint(jax.random.fold_in(rng, axis), (), 0, shape[axis]) for axis in range(len(shape))]
    values = values.at[tuple(index_at)].set(least)
    longest = shape.index(max(shape))
    index_at[longest] = (index_at[longest] + 1) % shape[longest]
    return values.at[tuple(index_at)].set(top_value)


def block_levels(key, extent, pieces, least, top_value):
    loudness = 1.0
    for axis_at, parts in pieces:
        steps = jax.random.uniform(jax.random.fold_in(jax.random.fold_in(key, 6), axis_at), (parts,), jnp.float32, least / len(pieces), top_value / len(pieces))
        loudness = loudness * jnp.repeat(jnp.exp(steps), extent[axis_at] // parts).reshape((-1,) + (1,) * (len(extent) - 1 - axis_at))
    return loudness


def normal_values(key, dims, deviation, reach, cuts=(), held_as=jnp.bfloat16):
    level = block_levels(key, dims, cuts, -0.22, 0.18) if cuts else 1.0
    array = jax.random.normal(key, dims, jnp.float32) * deviation * level
    return jnp.minimum(jnp.maximum(array, -reach), reach).astype(held_as)


def setup_inputs(seed: int = 0) -> dict:
    keys = jax.random.split(jax.random.key(seed), 9)
    return {
        "design": draw_design(jax.random.fold_in(keys[8], 71), 0),
        "nuisance_design": normal_values(keys[1], (OBS, NUIS), (OBS_DEV // 2) ** -0.5, 1.0, ((0, 32),)),
        "observed": normal_values(keys[2], (OBS,), 1.0, 6.0, ((0, 32),), jnp.float32),
        "arc_of_row": draw_arc_of_row(jax.random.fold_in(keys[8], 71), 0),
        "nuis_size": touch_ends(jax.random.randint(keys[4], (ARCS,), NUIS // 4, NUIS + 1), jax.random.fold_in(keys[4], 1), NUIS // 4, NUIS).astype(jnp.int32),
        "weight_index": touch_ends(jax.random.randint(keys[5], (OBS,), 0, KINDS), jax.random.fold_in(keys[5], 1), 0, KINDS - 1).astype(jnp.int32),
        "kind_weight": jnp.clip(jnp.exp(jax.random.uniform(keys[6], (KINDS,), jnp.float32, math.log(0.3), math.log(3.0))), 0.3, 3.0),
        "mission_weight": jnp.clip(jnp.exp(math.log(3.0) - 2.3025851 * jax.random.uniform(keys[7], (N_MISSION,), jnp.float32) ** block_levels(keys[7], (N_MISSION,), ((0, 2),), -0.2, 0.2)), 0.3, 3.0),
    }


def local_system(design, nuisance_design, observed, arc_of_row, nuis_size, weight_index, kind_weight):
    kind_ids = jnp.arange(kind_weight.shape[0], dtype=jnp.int32)
    row_weight = jnp.sum(jnp.where(weight_index[:, None] == kind_ids[None, :], kind_weight[None, :], 0.0), axis=1)
    nuis_ids = jnp.arange(nuisance_design.shape[1], dtype=jnp.int32)
    eye_block = jnp.eye(nuisance_design.shape[1], dtype=jnp.float32)
    blocks = []
    solved = []
    solved_obs = []
    for arc_id in range(ARCS_DEV):
        col_mask = (nuis_ids < nuis_size[arc_id]).astype(jnp.bfloat16)
        in_arc = (arc_of_row == arc_id).astype(jnp.float32)
        masked = nuisance_design * col_mask[None, :]
        weighted = (masked.astype(jnp.float32) * (row_weight * in_arc)[:, None]).astype(jnp.bfloat16)
        normal_ll = jnp.dot(weighted.T.astype(jnp.float32), masked.astype(jnp.float32), preferred_element_type=jnp.float32) + eye_block
        coupling = jnp.dot(weighted.T.astype(jnp.float32), design.astype(jnp.float32), preferred_element_type=jnp.float32)
        obs_part = jnp.dot(weighted.T.astype(jnp.float32), observed, precision=lax.Precision.HIGHEST)
        factor = jnp.linalg.cholesky(normal_ll)
        blocks.append(weighted)
        solved.append(jax.scipy.linalg.cho_solve((factor, True), coupling).astype(jnp.bfloat16))
        solved_obs.append(jax.scipy.linalg.cho_solve((factor, True), obs_part))
    stacked = jnp.concatenate(blocks, axis=1)
    solved_all = jnp.concatenate(solved, axis=0)
    obs_all = jnp.concatenate(solved_obs, axis=0)
    reduced = (row_weight[:, None] * design.astype(jnp.float32) - jnp.dot(stacked.astype(jnp.float32), solved_all.astype(jnp.float32), preferred_element_type=jnp.float32)).astype(jnp.bfloat16)
    reduced_obs = (row_weight * observed - jnp.dot(stacked.astype(jnp.float32), obs_all, precision=lax.Precision.HIGHEST)).astype(jnp.bfloat16)
    right_term = jnp.dot(reduced_obs.astype(jnp.float32), design.astype(jnp.float32), preferred_element_type=jnp.float32)
    half_width = design.shape[1] // 2
    tail_term = jnp.sum(design[:, half_width:].astype(jnp.float32) * reduced[:, half_width:].astype(jnp.float32), axis=0)
    return (reduced, right_term, tail_term)

def reference(design, nuisance_design, observed, arc_of_row, nuis_size, weight_index, kind_weight, mission_weight):
    devices = N_MISSION * N_ARC
    col_ids = jnp.arange(P_SIZE, dtype=jnp.int32)
    row_ids = jnp.arange(HALF, dtype=jnp.int32)
    keep_upper = col_ids[None, :] >= row_ids[:, None]

    def per_block(totals, block_id):
        fold_total, right_total, tail_total = totals
        row_start = (block_id * OBS_DEV).astype(jnp.int32)
        arc_start = (block_id * ARCS_DEV).astype(jnp.int32)
        block_design = lax.dynamic_slice_in_dim(design, row_start, OBS_DEV, 0)
        block_nuis = lax.dynamic_slice_in_dim(nuisance_design, row_start, OBS_DEV, 0)
        block_obs = lax.dynamic_slice_in_dim(observed, row_start, OBS_DEV, 0)
        block_arcs = lax.dynamic_slice_in_dim(arc_of_row, row_start, OBS_DEV, 0)
        block_kinds = lax.dynamic_slice_in_dim(weight_index, row_start, OBS_DEV, 0)
        block_sizes = lax.dynamic_slice_in_dim(nuis_size, arc_start, ARCS_DEV, 0)
        weight = mission_weight[block_id // N_ARC]
        reduced, right_term, tail_term = local_system(block_design, block_nuis, block_obs, block_arcs, block_sizes, block_kinds, kind_weight)
        term_full = weight * jnp.dot(block_design.T.astype(jnp.float32), reduced.astype(jnp.float32), preferred_element_type=jnp.float32)
        folded = jnp.where(keep_upper, term_full[:HALF], term_full[::-1, ::-1][:HALF])
        rounded = lax.optimization_barrier(folded.astype(jnp.bfloat16))
        fold_total = fold_total + rounded.astype(jnp.float32)
        return ((fold_total, right_total + weight * right_term, tail_total + weight * tail_term), None)
    initial = (jnp.zeros((HALF, P_SIZE), jnp.float32), jnp.zeros((P_SIZE,), jnp.float32), jnp.zeros((HALF,), jnp.float32))
    totals, unused_out = lax.scan(per_block, initial, jnp.arange(devices, dtype=jnp.int32))
    return (totals[0], totals[1], totals[2])
```

```python
import functools

import jax
import jax.numpy as jnp
import numpy as np
from jax import lax
from jax.experimental import pallas as pl
from jax.experimental.pallas import tpu as pltpu
from jax.sharding import PartitionSpec as P

LANES = 128


def rounded_up(value, unit):
    return -(-value // unit) * unit


def projector_kernel(
    sizes_ref, kinds_ref, nuis_ref, arc_col_ref, arc_row_ref, kind_col_ref, obs_row_ref, out_ref
):
    rows, wide = out_ref.shape
    arc_col = arc_col_ref[...]
    kind_col = kind_col_ref[...]
    weight = jnp.zeros((rows, 1), jnp.float32)
    for kind in range(kinds_ref.shape[0]):
        weight = jnp.where(kind_col == kind, kinds_ref[kind], weight)
    size = jnp.zeros((rows, 1), jnp.int32)
    for arc in range(sizes_ref.shape[0]):
        size = jnp.where(arc_col == arc, sizes_ref[arc], size)
    nuis = nuis_ref[...].astype(jnp.float32)
    nuis = jnp.where(lax.broadcasted_iota(jnp.int32, nuis.shape, 1) < size, nuis, 0.0)
    padded = jnp.concatenate(
        [nuis, jnp.zeros((wide - rows, nuis.shape[1]), jnp.float32)], axis=0
    )
    gram = lax.dot_general(
        nuis.astype(jnp.bfloat16),
        padded.astype(jnp.bfloat16),
        (((1,), (1,)), ((), ())),
        preferred_element_type=jnp.float32,
    )
    lane = lax.broadcasted_iota(jnp.int32, (rows, wide), 1)
    sub = lax.broadcasted_iota(jnp.int32, (rows, wide), 0)
    state = jnp.where(arc_col == arc_row_ref[...], gram, 0.0)
    state = state + jnp.where(lane == sub, 1.0 / weight, 0.0)
    for k in range(rows):
        row = state[k : k + 1, :]
        col = state[:, k : k + 1]
        inv = 1.0 / row[:, k : k + 1]
        scaled_row = row * inv
        scaled_col = col * inv
        swept = state - col * scaled_row
        swept = jnp.where(lane == k, scaled_col, swept)
        swept = jnp.where(sub == k, scaled_row, swept)
        state = jnp.where((lane == k) & (sub == k), -inv, swept)
    inverse = -state
    reduced_obs = jnp.sum(inverse * obs_row_ref[...], axis=1, keepdims=True)
    out_ref[...] = jnp.where(lane == rows, reduced_obs, inverse).astype(out_ref.dtype)


def fold_kernel(
    block_rows,
    width,
    with_right,
    weight_ref,
    span_ref,
    proj_ref,
    picked_ref,
    perm_ref,
    rows_ref,
    above_ref,
    mirror_ref,
    fold_ref,
    tail_ref,
    *rest,
):
    lhs_ref = rest[-1]
    tile = pl.program_id(0)
    tile_cols = above_ref.shape[1]
    out_rows = fold_ref.shape[0]
    weight = weight_ref[0]

    @pl.when(tile == 0)
    def _():
        tail = jnp.zeros((1, width), jnp.float32)
        lane = lax.broadcasted_iota(jnp.int32, (block_rows, width), 1)
        pieces = []
        for block in range(proj_ref.shape[0] // block_rows):
            span = pl.ds(block * block_rows, block_rows)
            proj = proj_ref[span, :]
            picked = picked_ref[span, :]
            reduced = lax.dot_general(
                proj[:, :block_rows], picked, (((1,), (0,)), ((), ())),
                preferred_element_type=jnp.float32,
            )
            tail_reduced = reduced[:, 2 * width :].astype(jnp.bfloat16).astype(jnp.float32)
            tail += jnp.sum(
                picked[:, 2 * width :].astype(jnp.float32) * tail_reduced, axis=0, keepdims=True
            )
            first = jnp.where(
                lane == width - 1,
                proj[:, block_rows : block_rows + 1].astype(jnp.float32),
                reduced[:, :width],
            )
            second = jnp.dot(
                reduced[:, width : 2 * width].astype(jnp.bfloat16),
                perm_ref[...],
                preferred_element_type=jnp.float32,
            )
            pieces.append(jnp.concatenate([first, second], axis=1))
        lhs_ref[...] = jnp.concatenate(pieces, axis=0).T.astype(jnp.bfloat16)
        tail_ref[...] = weight * tail

    low, high = span_ref[0], span_ref[1]
    col_start = tile * tile_cols
    all_above = col_start >= high
    all_mirror = col_start + tile_cols <= low

    def above_tile():
        return weight * jnp.dot(
            lhs_ref[pl.ds(0, width), :], above_ref[...], preferred_element_type=jnp.float32
        )

    def mirror_tile():
        mirror = jnp.dot(
            lhs_ref[pl.ds(width, rounded_up(out_rows, 16)), :],
            mirror_ref[...],
            preferred_element_type=jnp.float32,
        )[:out_rows]
        mirror = (weight * mirror).astype(jnp.bfloat16)
        flip = (
            lax.broadcasted_iota(jnp.int32, (LANES, LANES), 0)
            + lax.broadcasted_iota(jnp.int32, (LANES, LANES), 1)
            == LANES - 1
        ).astype(jnp.float32).astype(jnp.bfloat16)
        return jnp.concatenate(
            [
                jnp.dot(
                    mirror[:, start : start + LANES], flip, preferred_element_type=jnp.float32
                )
                for start in range(tile_cols - LANES, -1, -LANES)
            ],
            axis=1,
        )

    if with_right:
        above = above_tile()
        rest[0][...] = above[width - 1 : width, :]
        fold_ref[...] = above[:out_rows].astype(fold_ref.dtype)
    else:

        @pl.when(jnp.logical_not(all_mirror))
        def _():
            fold_ref[...] = above_tile()[:out_rows].astype(fold_ref.dtype)

    @pl.when(all_mirror)
    def _():
        fold_ref[...] = mirror_tile().astype(fold_ref.dtype)

    @pl.when(jnp.logical_not(jnp.logical_or(all_above, all_mirror)))
    def _():
        cols = lax.broadcasted_iota(jnp.int32, (out_rows, tile_cols), 1) + col_start
        fold_ref[...] = jnp.where(
            cols >= rows_ref[...], fold_ref[...].astype(jnp.float32), mirror_tile()
        ).astype(fold_ref.dtype)


def on_any_mesh(
    design,
    nuisance_design,
    observed,
    arc_of_row,
    nuis_size,
    weight_index,
    kind_weight,
    mission_weight,
):
    groups = lax.axis_size("mission")
    members = lax.axis_size("arc")
    group = lax.axis_index("mission")
    member = lax.axis_index("arc")
    block_rows, width_all = design.shape
    half_width = width_all // 2
    final_rows = half_width // (groups * members)
    wide = rounded_up(block_rows + 1, LANES)
    inner = 2 if members % 2 == 0 else 1
    outer = 4 if members % (4 * inner) == 0 else 1
    mid = members // (outer * inner)
    mid_at = (member // inner) % mid
    gather_groups = [
        [(o * mid + y) * inner + c for o in range(outer) for c in range(inner)]
        for y in range(mid)
    ]

    def gathered(array):
        return lax.all_gather(
            array, "arc", axis=0, tiled=True, axis_index_groups=gather_groups
        )

    def member_of(y):
        return (member // (inner * mid) * mid + y) * inner + member % inner

    vmem = pl.BlockSpec(memory_space=pltpu.VMEM)
    smem = pl.BlockSpec(memory_space=pltpu.SMEM)

    design_all = gathered(design)

    proj = pl.pallas_call(
        projector_kernel,
        out_shape=jax.ShapeDtypeStruct((block_rows, wide), jnp.bfloat16),
        in_specs=[smem, smem, vmem, vmem, vmem, vmem, vmem],
        out_specs=vmem,
        cost_estimate=pl.CostEstimate(flops=10_000_000, bytes_accessed=100_000, transcendentals=0),
        name="projector",
    )(
        nuis_size,
        kind_weight,
        nuisance_design,
        arc_of_row[:, None],
        jnp.pad(arc_of_row, (0, wide - block_rows), constant_values=-1)[None, :],
        weight_index[:, None],
        jnp.pad(observed, (0, wide - block_rows))[None, :],
    )
    proj_all = gathered(proj)

    shifts = [(dm, dy) for dm in range(groups) for dy in range(mid)]
    shifts.sort(key=lambda shift: (shift[0] == 0, shift[1] == 0))
    per_call = max(1, len(shifts) // 2)
    out_rows = per_call * final_rows
    width = rounded_up(out_rows + 1, LANES)
    place = np.arange(out_rows)
    perm = np.zeros((width, width), np.float32)
    perm[(place // final_rows) * final_rows + final_rows - 1 - place % final_rows, place] = 1.0
    tile_cols = 512
    tiles = width_all // tile_cols
    all_rows = design_all.shape[0]
    right_cols = width_all // (groups * members)
    whole = lambda shape: pl.BlockSpec(shape, lambda j: (0, 0))

    def fold_call(owners, with_right):
        def picked(start_of):
            parts = [
                lax.dynamic_slice_in_dim(design_all, start_of(owner), final_rows, 1)
                for owner in owners
            ]
            blank = jnp.zeros((all_rows, width - out_rows), design_all.dtype)
            return parts + [blank]

        picked_all = jnp.concatenate(
            picked(lambda block: block * final_rows)
            + picked(lambda block: width_all - (block + 1) * final_rows)
            + picked(lambda block: half_width + block * final_rows),
            axis=1,
        )
        starts = jnp.stack(owners).astype(jnp.int32) * final_rows
        row_ids = (
            starts[:, None] + jnp.arange(final_rows, dtype=jnp.int32)[None, :]
        ).reshape(out_rows, 1)
        span = jnp.stack([jnp.min(starts), jnp.max(starts) + final_rows - 1])
        out_shape = [
            jax.ShapeDtypeStruct((out_rows, width_all), jnp.bfloat16),
            jax.ShapeDtypeStruct((1, width), jnp.float32),
        ]
        out_specs = [
            pl.BlockSpec((out_rows, tile_cols), lambda j: (0, j)),
            whole((1, width)),
        ]
        if with_right:
            out_shape.append(jax.ShapeDtypeStruct((1, width_all), jnp.float32))
            out_specs.append(pl.BlockSpec((1, tile_cols), lambda j: (0, j)))
        return pl.pallas_call(
            functools.partial(fold_kernel, block_rows, width, with_right),
            grid=(tiles,),
            out_shape=tuple(out_shape),
            in_specs=[
                smem,
                smem,
                whole((all_rows, wide)),
                whole((all_rows, 3 * width)),
                whole((width, width)),
                whole((out_rows, 1)),
                pl.BlockSpec((all_rows, tile_cols), lambda j: (0, j)),
                pl.BlockSpec((all_rows, tile_cols), lambda j: (0, tiles - 1 - j)),
            ],
            out_specs=tuple(out_specs),
            scratch_shapes=[pltpu.VMEM((2 * width, all_rows), jnp.bfloat16)],
            compiler_params=pltpu.CompilerParams(
                dimension_semantics=("arbitrary",), vmem_limit_bytes=60 * 2**20
            ),
            cost_estimate=pl.CostEstimate(
                flops=4 * width * all_rows * width_all,
                bytes_accessed=4 * all_rows * width_all,
                transcendentals=0,
            ),
            name="fold",
        )(
            mission_weight,
            span,
            proj_all,
            picked_all,
            jnp.asarray(perm, jnp.bfloat16),
            row_ids,
            design_all,
            design_all,
        )

    def ring(dm, dy):
        pairs = []
        for m in range(groups):
            for a in range(members):
                o, y, c = a // (inner * mid), (a // inner) % mid, a % inner
                target = (o * mid + (y + dy) % mid) * inner + c
                pairs.append((m * members + a, (m + dm) % groups * members + target))
        return pairs

    right = None
    folds, vectors = [], []
    for first in range(0, len(shifts), per_call):
        here = shifts[first : first + per_call]
        owners = [
            (group + dm) % groups * members + member_of((mid_at + dy) % mid) for dm, dy in here
        ]
        fold, tail, *extra = fold_call(owners, right is None)
        if right is None:
            right = extra[0][0]
        for at, (dm, dy) in enumerate(here):
            rows = slice(at * final_rows, (at + 1) * final_rows)
            block = fold[rows]
            vector = jnp.concatenate(
                [
                    lax.dynamic_slice_in_dim(right, owners[at] * right_cols, right_cols),
                    tail[0, rows],
                ]
            )
            if dm or dy:
                block = lax.ppermute(block, ("mission", "arc"), ring(dm, dy))
                vector = lax.ppermute(vector, ("mission", "arc"), ring(dm, dy))
            folds.append(block.astype(jnp.float32))
            vectors.append(vector)
    fold_total = functools.reduce(jnp.add, folds)
    vector_total = functools.reduce(jnp.add, vectors)
    return (fold_total, vector_total[:right_cols], vector_total[right_cols:])


TILES = 8
ARRIVAL = (0, 2, 7, 5, 6, 4, 3, 1)
SWAPPED = tuple(ARRIVAL.index(tile ^ 1) for tile in ARRIVAL)
EARLY_Z = 3
EARLY_X = 5


def tile_at(slot, half):
    tile = ARRIVAL[slot]
    return tile + half * (1 - 2 * (tile % 2))


def slot_of(tile, half):
    return ARRIVAL.index(tile ^ half)


def flip_matrix(size):
    return (
        (
            lax.broadcasted_iota(jnp.int32, (size, size), 0)
            + lax.broadcasted_iota(jnp.int32, (size, size), 1)
            == size - 1
        )
        .astype(jnp.float32)
        .astype(jnp.bfloat16)
    )


def weighted_projector(sizes_ref, kinds_ref, weight_ref, nuis_ref, arc_ref, kind_ref, obs_ref):
    rows = nuis_ref.shape[0]
    wide = arc_ref.shape[1]
    lane = lax.broadcasted_iota(jnp.int32, (rows, wide), 1)
    sub = lax.broadcasted_iota(jnp.int32, (rows, wide), 0)
    arc_row = arc_ref[...].astype(jnp.float32)
    kind_row = kind_ref[...]
    scale_row = jnp.ones((1, wide), jnp.float32)
    for kind in range(kinds_ref.shape[0]):
        scale_row = jnp.where(kind_row == kind, 1.0 / kinds_ref[kind], scale_row)
    arc_col = jnp.sum(jnp.where(lane == sub, arc_row, 0.0), axis=1, keepdims=True)
    size = jnp.zeros((rows, 1), jnp.int32)
    for arc in range(sizes_ref.shape[0]):
        size = jnp.where(arc_col == arc, sizes_ref[arc], size)
    nuis = nuis_ref[...].astype(jnp.float32)
    nuis = jnp.where(lax.broadcasted_iota(jnp.int32, nuis.shape, 1) < size, nuis, 0.0)
    padded = jnp.concatenate(
        [nuis, jnp.zeros((wide - rows, nuis.shape[1]), jnp.float32)], axis=0
    )
    gram = lax.dot_general(
        nuis.astype(jnp.bfloat16),
        padded.astype(jnp.bfloat16),
        (((1,), (1,)), ((), ())),
        preferred_element_type=jnp.float32,
    )
    state = jnp.where(arc_col == arc_row, gram, 0.0)
    state = state + jnp.where(lane == sub, scale_row, 0.0)
    for k in range(rows):
        row = state[k : k + 1, :]
        col = state[:, k : k + 1]
        inv = 1.0 / row[:, k : k + 1]
        scaled_row = row * inv
        scaled_col = col * inv
        swept = state - col * scaled_row
        swept = jnp.where(lane == k, scaled_col, swept)
        swept = jnp.where(sub == k, scaled_row, swept)
        state = jnp.where((lane == k) & (sub == k), -inv, swept)
    inverse = state * -weight_ref[0]
    reduced_obs = jnp.sum(
        jnp.where(lane < rows, inverse * obs_ref[...], 0.0), axis=1, keepdims=True
    )
    return jnp.where(lane == rows, reduced_obs, inverse).astype(jnp.bfloat16)


def normals_kernel(
    sizes_ref, kinds_ref, weight_ref, design_ref, nuis_ref, arc_ref, kind_ref, obs_ref,
    fold_ref, vec_out_ref,
    gath, proj, turned, lhs, right_lhs, part, first_in, second_out, second_in, vec, vec_in,
    own_sem, z_send, z_recv, x_send, x_recv, r_send, r_recv, d_send, d_recv,
    one_send, one_recv, two_send, two_recv, v_send, v_recv,
):
    rows = nuis_ref.shape[0]
    tile_cols = gath.shape[2]
    mission = lax.axis_index("mission")
    arc = lax.axis_index("arc")
    core = lax.rem(arc, 2)
    y = lax.rem(lax.div(arc, 2), 2)
    near = lax.rem(lax.div(arc, 4), 2)
    half = lax.div(arc, 8)
    group = 2 * mission + half

    def device(x=None, zh=None, zl=None, yy=None, c=None):
        x = mission if x is None else x
        zh = half if zh is None else zh
        zl = near if zl is None else zl
        yy = y if yy is None else yy
        c = core if c is None else c
        return (x, ((zh * 2 + zl) * 2 + yy) * 2 + c)

    x_peer = device(x=1 - mission)
    z_peer = device(zh=1 - half)
    sibling = device(c=1 - core)
    y_peer = device(yy=1 - y)
    near_peer = device(zl=1 - near)
    cross_peer = device(zl=1 - near, yy=1 - y)

    def block(slot, at):
        span = pl.ds(at * rows, rows)
        return proj.at[span] if slot == TILES else gath.at[slot, span]

    def remote(src, dst, send, recv, target):
        return pltpu.make_async_remote_copy(
            src_ref=src,
            dst_ref=dst,
            send_sem=send,
            recv_sem=recv,
            device_id=target,
            device_id_type=pl.DeviceIdType.MESH,
        )

    def z_copy(slot):
        source = slot if slot == TILES else SWAPPED[slot]
        return remote(block(source, 0), block(slot, 2), z_send.at[slot], z_recv.at[slot], z_peer)

    def x_copy(slot):
        return remote(block(slot, 0), block(slot, 4), x_send.at[slot], x_recv.at[slot], x_peer)

    def relay(slot):
        return remote(block(slot, 2), block(slot, 6), r_send.at[slot], r_recv.at[slot], x_peer)

    def share(chip, slot):
        return remote(
            block(slot, 2 * chip),
            block(slot, 2 * chip + 1),
            d_send.at[chip, slot],
            d_recv.at[chip, slot],
            sibling,
        )

    def own_copy(slot):
        start = tile_at(slot, half) * tile_cols
        return pltpu.make_async_copy(
            design_ref.at[:, pl.ds(pl.multiple_of(start, LANES), tile_cols)],
            block(slot, 0),
            own_sem.at[slot],
        )

    def stage_one(n):
        if n % 2 == 0:
            src, target = part.at[n, :, 1 - y], y_peer
        else:
            src, target = part.at[n, 1 - near], near_peer
        return remote(src, first_in.at[n], one_send.at[n], one_recv.at[n], target)

    def stage_two(n):
        target = near_peer if n % 2 == 0 else y_peer
        return remote(
            second_out.at[n], second_in.at[n], two_send.at[n], two_recv.at[n], target
        )

    def held(n, mine):
        if n % 2 == 0:
            at = near if mine else 1 - near
            return part[n, at, y].astype(jnp.float32) + first_in[n, at].astype(jnp.float32)
        at = y if mine else 1 - y
        return part[n, near, at].astype(jnp.float32) + first_in[n, at].astype(jnp.float32)

    def vector_copy(k):
        target = (y_peer, near_peer, cross_peer)[k]
        return remote(vec, vec_in.at[k], v_send.at[k], v_recv.at[k], target)

    for slot in range(TILES):
        own_copy(slot).start()
    barrier = pltpu.get_barrier_semaphore()
    peers = (x_peer, z_peer, sibling, y_peer, near_peer, cross_peer)
    for peer in peers:
        pl.semaphore_signal(barrier, inc=1, device_id=peer, device_id_type=pl.DeviceIdType.MESH)
    pl.semaphore_wait(barrier, len(peers))
    for slot in range(TILES):
        own_copy(slot).wait()
    for slot in range(EARLY_Z):
        z_copy(slot).start()
    for slot in range(EARLY_X):
        x_copy(slot).start()
    for slot in range(TILES):
        share(0, slot).start()

    proj[pl.ds(0, rows), :] = weighted_projector(
        sizes_ref, kinds_ref, weight_ref, nuis_ref, arc_ref, kind_ref, obs_ref
    )
    z_copy(TILES).start()
    x_copy(TILES).start()
    share(0, TILES).start()
    for slot in range(EARLY_Z, TILES):
        z_copy(slot).start()

    def from_z(slot):
        z_copy(slot).wait_recv()
        relay(slot).start()
        share(1, slot).start()

    def from_x(slot):
        x_copy(slot).wait_recv()
        share(2, slot).start()

    def from_relay(slot):
        relay(slot).wait_recv()
        share(3, slot).start()

    def settled(slot):
        for chip in range(4):
            share(chip, slot).wait_recv()

    def solved(slot):
        return jnp.concatenate(
            [
                jnp.dot(
                    proj[pl.ds(at * rows, rows), :][:, :rows],
                    gath[slot, pl.ds(at * rows, rows), :],
                    preferred_element_type=jnp.float32,
                )
                for at in range(2 * 4)
            ],
            axis=0,
        )

    def make_lhs(mirrored):
        turned[...] = solved(mission + 2 * mirrored).T.astype(jnp.bfloat16)
        for to in range(4):
            start = 2 * rows * to + rows * core
            if mirrored:
                start = tile_cols - rows - start
            picked = turned[pl.ds(pl.multiple_of(start, 16), rows), :]
            if mirrored:
                picked = jnp.dot(
                    flip_matrix(rows), picked, preferred_element_type=jnp.float32
                ).astype(jnp.bfloat16)
            lhs[mirrored, pl.ds(to * rows, rows), :] = picked

    def product(mirrored, slot):
        out = jnp.dot(lhs[mirrored], gath[slot], preferred_element_type=jnp.float32)
        if not mirrored:
            return out
        flip = flip_matrix(LANES)
        out = out.astype(jnp.bfloat16)
        return jnp.concatenate(
            [
                jnp.dot(out[:, start : start + LANES], flip, preferred_element_type=jnp.float32)
                for start in range(tile_cols - LANES, -1, -LANES)
            ],
            axis=1,
        )

    def put(n, value):
        part[n] = value.astype(jnp.bfloat16).reshape(2, 2, rows, tile_cols)

    def either(n, mirror_when, mirror_slot, above_slot):
        @pl.when(mirror_when)
        def _():
            put(n, product(1, mirror_slot))

        @pl.when(jnp.logical_not(mirror_when))
        def _():
            put(n, product(0, above_slot))

    def job(n):
        if n == 0:
            put(n, product(0, 1 + mission))
        elif n == 1:
            put(n, product(0, 2 + mission))
        elif n == 2:
            either(n, mission == 1, 2, 3)
        elif n == 3:
            local = lax.broadcasted_iota(jnp.int32, (4 * rows, tile_cols), 0)
            local = lax.div(local, rows) * (2 * rows) + lax.rem(local, rows) + rows * core
            cols = lax.broadcasted_iota(jnp.int32, (4 * rows, tile_cols), 1)
            put(n, jnp.where(cols >= local, product(0, mission), product(1, 2 + mission)))
        elif n == 4:
            put(n, product(0, 4))
        elif n == 5:
            either(n, mission == 1, 4, 5)
        elif n == 6:
            put(n, product(0, 6 - mission))
        else:
            either(n, half == 1, 4 + mission, 7 - mission)
        stage_one(n).start()

    def out_tile(n):
        def above(slot):
            return tile_at(slot, half)

        def mirror(slot):
            return TILES - 1 - tile_at(slot, half)

        def by_mission(low, high):
            return low + mission * (high - low)

        return (
            lambda: by_mission(above(1), above(2)),
            lambda: by_mission(above(2), above(3)),
            lambda: by_mission(above(3), mirror(2)),
            lambda: group,
            lambda: above(4),
            lambda: by_mission(above(5), mirror(4)),
            lambda: by_mission(above(6), above(5)),
            lambda: by_mission(
                above(7) + half * (mirror(4) - above(7)),
                above(6) + half * (mirror(5) - above(6)),
            ),
        )[n]()

    def pass_on(n):
        stage_one(n).wait_recv()
        second_out[n] = held(n, False).astype(jnp.bfloat16)
        stage_two(n).start()

    def finish(n):
        stage_two(n).wait_recv()
        start = pl.multiple_of(out_tile(n) * tile_cols, LANES)
        fold_ref[:, pl.ds(start, tile_cols)] = held(n, True) + second_in[n].astype(jnp.float32)

    def vectors():
        def by_place(a, b, c, d):
            return (1 - half) * (a + mission * (b - a)) + half * (c + mission * (d - c))

        low = by_place(
            slot_of(0, 0), slot_of(4, 0), slot_of(2, 1), slot_of(6, 1)
        )
        high = by_place(
            slot_of(1, 0), slot_of(5, 0), slot_of(3, 1), slot_of(7, 1)
        )
        last = by_place(
            slot_of(4, 0), slot_of(6, 0), slot_of(5, 1), slot_of(7, 1)
        )
        lines = [
            jnp.dot(right_lhs[...], gath[slot], preferred_element_type=jnp.float32)[:1]
            for slot in (low, high)
        ]
        reduced = solved(last).astype(jnp.bfloat16).astype(jnp.float32)
        lines.append(
            jnp.sum(gath[last].astype(jnp.float32) * reduced, axis=0, keepdims=True)
        )
        at = 0
        for line in lines:
            for start in range(0, tile_cols, LANES):
                vec[at : at + 1, :] = line[:, start : start + LANES]
                at += 1
        vec[at:, :] = jnp.zeros((vec.shape[0] - at, LANES), jnp.float32)
        for k in range(3):
            vector_copy(k).start()

    from_z(0)
    from_z(1)
    for slot in range(EARLY_X, TILES):
        x_copy(slot).start()
    for slot in range(3):
        from_x(slot)
    from_z(2)
    from_z(TILES)
    from_x(TILES)
    from_relay(0)
    from_relay(1)
    from_x(3)
    from_relay(TILES)
    from_relay(2)
    settled(0)
    settled(1)
    settled(TILES)
    make_lhs(0)
    right_lhs[...] = proj[...].astype(jnp.float32).T.astype(jnp.bfloat16)[rows : rows + 16]
    settled(2)
    job(0)
    from_z(3)
    from_relay(3)
    settled(3)
    job(1)
    make_lhs(1)
    job(2)
    job(3)
    for slot in range(4, TILES):
        from_x(slot)
    from_z(4)
    from_relay(4)
    settled(4)
    job(4)
    pass_on(0)
    pass_on(1)
    from_z(5)
    from_relay(5)
    settled(5)
    job(5)
    pass_on(2)
    pass_on(3)
    finish(0)
    from_z(6)
    from_relay(6)
    settled(6)
    job(6)
    pass_on(4)
    finish(1)
    finish(2)
    from_z(7)
    from_relay(7)
    settled(7)
    job(7)
    vectors()
    pass_on(5)
    finish(3)
    finish(4)
    pass_on(6)
    finish(5)
    pass_on(7)
    finish(6)
    total = vec[...]
    for k in range(3):
        vector_copy(k).wait_recv()
        total = total + vec_in[k]
    vec_out_ref[...] = total
    finish(7)

    for slot in range(TILES + 1):
        z_copy(slot).wait_send()
        x_copy(slot).wait_send()
        relay(slot).wait_send()
        for chip in range(4):
            share(chip, slot).wait_send()
    for n in range(TILES):
        stage_one(n).wait_send()
        stage_two(n).wait_send()
    for k in range(3):
        vector_copy(k).wait_send()


def on_paired_chips(
    design,
    nuisance_design,
    observed,
    arc_of_row,
    nuis_size,
    weight_index,
    kind_weight,
    mission_weight,
):
    rows, width_all = design.shape
    wide = rounded_up(rows + 1, LANES)
    tile_cols = width_all // TILES
    stacked = 2 * 4 * rows
    vec_rows = rounded_up(3 * tile_cols // LANES, 8)
    vmem = pl.BlockSpec(memory_space=pltpu.VMEM)
    smem = pl.BlockSpec(memory_space=pltpu.SMEM)
    dma = pltpu.SemaphoreType.DMA
    slots = TILES + 1

    def line(array, fill):
        return jnp.pad(array, (0, wide - rows), constant_values=fill)[None, :]

    fold, vec = pl.pallas_call(
        normals_kernel,
        out_shape=(
            jax.ShapeDtypeStruct((rows, width_all), jnp.float32),
            jax.ShapeDtypeStruct((vec_rows, LANES), jnp.float32),
        ),
        in_specs=[smem, smem, smem, pl.BlockSpec(memory_space=pl.ANY), vmem, vmem, vmem, vmem],
        out_specs=(vmem, vmem),
        scratch_shapes=[
            pltpu.VMEM((TILES, stacked, tile_cols), jnp.bfloat16),
            pltpu.VMEM((stacked, wide), jnp.bfloat16),
            pltpu.VMEM((tile_cols, stacked), jnp.bfloat16),
            pltpu.VMEM((2, 4 * rows, stacked), jnp.bfloat16),
            pltpu.VMEM((16, stacked), jnp.bfloat16),
            pltpu.VMEM((TILES, 2, 2, rows, tile_cols), jnp.bfloat16),
            pltpu.VMEM((TILES, 2, rows, tile_cols), jnp.bfloat16),
            pltpu.VMEM((TILES, rows, tile_cols), jnp.bfloat16),
            pltpu.VMEM((TILES, rows, tile_cols), jnp.bfloat16),
            pltpu.VMEM((vec_rows, LANES), jnp.float32),
            pltpu.VMEM((3, vec_rows, LANES), jnp.float32),
            dma((TILES,)),
            dma((slots,)),
            dma((slots,)),
            dma((slots,)),
            dma((slots,)),
            dma((slots,)),
            dma((slots,)),
            dma((4, slots)),
            dma((4, slots)),
            dma((TILES,)),
            dma((TILES,)),
            dma((TILES,)),
            dma((TILES,)),
            dma((3,)),
            dma((3,)),
        ],
        compiler_params=pltpu.CompilerParams(
            collective_id=0, has_side_effects=True, vmem_limit_bytes=60 * 2**20
        ),
        name="normals",
    )(
        nuis_size,
        kind_weight,
        mission_weight,
        design,
        nuisance_design,
        line(arc_of_row, -1),
        line(weight_index, -1),
        line(observed, 0),
    )
    member = lax.rem(lax.axis_index("arc"), 8)
    right_cols = 2 * rows
    flat = vec.reshape(-1)
    right = lax.dynamic_slice_in_dim(flat, member * right_cols, right_cols)
    tail = lax.dynamic_slice_in_dim(flat, 2 * tile_cols + member * rows, rows)
    return fold, right, tail


def solution(mesh):
    placed = (
        P(("mission", "arc"), None),
        P(("mission", "arc"), None),
        P(("mission", "arc")),
        P(("mission", "arc")),
        P(("mission", "arc")),
        P(("mission", "arc")),
        P(),
        P("mission"),
    )

    def on_device(design, *rest):
        devices = lax.axis_size("mission") * lax.axis_size("arc")
        paired = lax.axis_size("mission") == 2 and lax.axis_size("arc") == 16
        rows, width_all = design.shape
        if paired and width_all == 2 * devices * rows and rows % 16 == 0 and width_all % (TILES * LANES) == 0:
            return on_paired_chips(design, *rest)
        return on_any_mesh(design, *rest)

    return jax.shard_map(
        on_device,
        mesh=mesh,
        in_specs=placed,
        out_specs=(P(("mission", "arc"), None), P(("mission", "arc")), P(("mission", "arc"))),
        check_vma=False,
    )
```

```python
import functools

import jax
import jax.numpy as jnp
import numpy as np
from jax import lax
from jax.experimental import pallas as pl
from jax.experimental.pallas import tpu as pltpu
from jax.sharding import PartitionSpec as P

LANES = 128


def rounded_up(value, unit):
    return -(-value // unit) * unit


def projector_kernel(
    sizes_ref, kinds_ref, nuis_ref, arc_col_ref, arc_row_ref, kind_col_ref, obs_row_ref, out_ref
):
    rows, wide = out_ref.shape
    arc_col = arc_col_ref[...]
    kind_col = kind_col_ref[...]
    weight = jnp.zeros((rows, 1), jnp.float32)
    for kind in range(kinds_ref.shape[0]):
        weight = jnp.where(kind_col == kind, kinds_ref[kind], weight)
    size = jnp.zeros((rows, 1), jnp.int32)
    for arc in range(sizes_ref.shape[0]):
        size = jnp.where(arc_col == arc, sizes_ref[arc], size)
    nuis = nuis_ref[...].astype(jnp.float32)
    nuis = jnp.where(lax.broadcasted_iota(jnp.int32, nuis.shape, 1) < size, nuis, 0.0)
    padded = jnp.concatenate(
        [nuis, jnp.zeros((wide - rows, nuis.shape[1]), jnp.float32)], axis=0
    )
    gram = lax.dot_general(
        nuis.astype(jnp.bfloat16),
        padded.astype(jnp.bfloat16),
        (((1,), (1,)), ((), ())),
        preferred_element_type=jnp.float32,
    )
    lane = lax.broadcasted_iota(jnp.int32, (rows, wide), 1)
    sub = lax.broadcasted_iota(jnp.int32, (rows, wide), 0)
    state = jnp.where(arc_col == arc_row_ref[...], gram, 0.0)
    state = state + jnp.where(lane == sub, 1.0 / weight, 0.0)
    for k in range(rows):
        row = state[k : k + 1, :]
        col = state[:, k : k + 1]
        inv = 1.0 / row[:, k : k + 1]
        scaled_row = row * inv
        scaled_col = col * inv
        swept = state - col * scaled_row
        swept = jnp.where(lane == k, scaled_col, swept)
        swept = jnp.where(sub == k, scaled_row, swept)
        state = jnp.where((lane == k) & (sub == k), -inv, swept)
    inverse = -state
    reduced_obs = jnp.sum(inverse * obs_row_ref[...], axis=1, keepdims=True)
    out_ref[...] = jnp.where(lane == rows, reduced_obs, inverse).astype(out_ref.dtype)


def fold_kernel(
    block_rows,
    width,
    with_right,
    weight_ref,
    span_ref,
    proj_ref,
    picked_ref,
    perm_ref,
    rows_ref,
    above_ref,
    mirror_ref,
    fold_ref,
    tail_ref,
    *rest,
):
    lhs_ref = rest[-1]
    tile = pl.program_id(0)
    tile_cols = above_ref.shape[1]
    out_rows = fold_ref.shape[0]
    weight = weight_ref[0]

    @pl.when(tile == 0)
    def _():
        tail = jnp.zeros((1, width), jnp.float32)
        lane = lax.broadcasted_iota(jnp.int32, (block_rows, width), 1)
        pieces = []
        for block in range(proj_ref.shape[0] // block_rows):
            span = pl.ds(block * block_rows, block_rows)
            proj = proj_ref[span, :]
            picked = picked_ref[span, :]
            reduced = lax.dot_general(
                proj[:, :block_rows], picked, (((1,), (0,)), ((), ())),
                preferred_element_type=jnp.float32,
            )
            tail_reduced = reduced[:, 2 * width :].astype(jnp.bfloat16).astype(jnp.float32)
            tail += jnp.sum(
                picked[:, 2 * width :].astype(jnp.float32) * tail_reduced, axis=0, keepdims=True
            )
            first = jnp.where(
                lane == width - 1,
                proj[:, block_rows : block_rows + 1].astype(jnp.float32),
                reduced[:, :width],
            )
            second = jnp.dot(
                reduced[:, width : 2 * width].astype(jnp.bfloat16),
                perm_ref[...],
                preferred_element_type=jnp.float32,
            )
            pieces.append(jnp.concatenate([first, second], axis=1))
        lhs_ref[...] = jnp.concatenate(pieces, axis=0).T.astype(jnp.bfloat16)
        tail_ref[...] = weight * tail

    low, high = span_ref[0], span_ref[1]
    col_start = tile * tile_cols
    all_above = col_start >= high
    all_mirror = col_start + tile_cols <= low

    def above_tile():
        return weight * jnp.dot(
            lhs_ref[pl.ds(0, width), :], above_ref[...], preferred_element_type=jnp.float32
        )

    def mirror_tile():
        mirror = jnp.dot(
            lhs_ref[pl.ds(width, rounded_up(out_rows, 16)), :],
            mirror_ref[...],
            preferred_element_type=jnp.float32,
        )[:out_rows]
        mirror = (weight * mirror).astype(jnp.bfloat16)
        flip = (
            lax.broadcasted_iota(jnp.int32, (LANES, LANES), 0)
            + lax.broadcasted_iota(jnp.int32, (LANES, LANES), 1)
            == LANES - 1
        ).astype(jnp.float32).astype(jnp.bfloat16)
        return jnp.concatenate(
            [
                jnp.dot(
                    mirror[:, start : start + LANES], flip, preferred_element_type=jnp.float32
                )
                for start in range(tile_cols - LANES, -1, -LANES)
            ],
            axis=1,
        )

    if with_right:
        above = above_tile()
        rest[0][...] = above[width - 1 : width, :]
        fold_ref[...] = above[:out_rows].astype(fold_ref.dtype)
    else:

        @pl.when(jnp.logical_not(all_mirror))
        def _():
            fold_ref[...] = above_tile()[:out_rows].astype(fold_ref.dtype)

    @pl.when(all_mirror)
    def _():
        fold_ref[...] = mirror_tile().astype(fold_ref.dtype)

    @pl.when(jnp.logical_not(jnp.logical_or(all_above, all_mirror)))
    def _():
        cols = lax.broadcasted_iota(jnp.int32, (out_rows, tile_cols), 1) + col_start
        fold_ref[...] = jnp.where(
            cols >= rows_ref[...], fold_ref[...].astype(jnp.float32), mirror_tile()
        ).astype(fold_ref.dtype)


def on_any_mesh(
    design,
    nuisance_design,
    observed,
    arc_of_row,
    nuis_size,
    weight_index,
    kind_weight,
    mission_weight,
):
    groups = lax.axis_size("mission")
    members = lax.axis_size("arc")
    group = lax.axis_index("mission")
    member = lax.axis_index("arc")
    block_rows, width_all = design.shape
    half_width = width_all // 2
    final_rows = half_width // (groups * members)
    wide = rounded_up(block_rows + 1, LANES)
    inner = 2 if members % 2 == 0 else 1
    outer = 4 if members % (4 * inner) == 0 else 1
    mid = members // (outer * inner)
    mid_at = (member // inner) % mid
    gather_groups = [
        [(o * mid + y) * inner + c for o in range(outer) for c in range(inner)]
        for y in range(mid)
    ]

    def gathered(array):
        return lax.all_gather(
            array, "arc", axis=0, tiled=True, axis_index_groups=gather_groups
        )

    def member_of(y):
        return (member // (inner * mid) * mid + y) * inner + member % inner

    vmem = pl.BlockSpec(memory_space=pltpu.VMEM)
    smem = pl.BlockSpec(memory_space=pltpu.SMEM)

    design_all = gathered(design)

    proj = pl.pallas_call(
        projector_kernel,
        out_shape=jax.ShapeDtypeStruct((block_rows, wide), jnp.bfloat16),
        in_specs=[smem, smem, vmem, vmem, vmem, vmem, vmem],
        out_specs=vmem,
        cost_estimate=pl.CostEstimate(flops=10_000_000, bytes_accessed=100_000, transcendentals=0),
        name="projector",
    )(
        nuis_size,
        kind_weight,
        nuisance_design,
        arc_of_row[:, None],
        jnp.pad(arc_of_row, (0, wide - block_rows), constant_values=-1)[None, :],
        weight_index[:, None],
        jnp.pad(observed, (0, wide - block_rows))[None, :],
    )
    proj_all = gathered(proj)

    shifts = [(dm, dy) for dm in range(groups) for dy in range(mid)]
    shifts.sort(key=lambda shift: (shift[0] == 0, shift[1] == 0))
    per_call = max(1, len(shifts) // 2)
    out_rows = per_call * final_rows
    width = rounded_up(out_rows + 1, LANES)
    place = np.arange(out_rows)
    perm = np.zeros((width, width), np.float32)
    perm[(place // final_rows) * final_rows + final_rows - 1 - place % final_rows, place] = 1.0
    tile_cols = 512
    tiles = width_all // tile_cols
    all_rows = design_all.shape[0]
    right_cols = width_all // (groups * members)
    whole = lambda shape: pl.BlockSpec(shape, lambda j: (0, 0))

    def fold_call(owners, with_right):
        def picked(start_of):
            parts = [
                lax.dynamic_slice_in_dim(design_all, start_of(owner), final_rows, 1)
                for owner in owners
            ]
            blank = jnp.zeros((all_rows, width - out_rows), design_all.dtype)
            return parts + [blank]

        picked_all = jnp.concatenate(
            picked(lambda block: block * final_rows)
            + picked(lambda block: width_all - (block + 1) * final_rows)
            + picked(lambda block: half_width + block * final_rows),
            axis=1,
        )
        starts = jnp.stack(owners).astype(jnp.int32) * final_rows
        row_ids = (
            starts[:, None] + jnp.arange(final_rows, dtype=jnp.int32)[None, :]
        ).reshape(out_rows, 1)
        span = jnp.stack([jnp.min(starts), jnp.max(starts) + final_rows - 1])
        out_shape = [
            jax.ShapeDtypeStruct((out_rows, width_all), jnp.bfloat16),
            jax.ShapeDtypeStruct((1, width), jnp.float32),
        ]
        out_specs = [
            pl.BlockSpec((out_rows, tile_cols), lambda j: (0, j)),
            whole((1, width)),
        ]
        if with_right:
            out_shape.append(jax.ShapeDtypeStruct((1, width_all), jnp.float32))
            out_specs.append(pl.BlockSpec((1, tile_cols), lambda j: (0, j)))
        return pl.pallas_call(
            functools.partial(fold_kernel, block_rows, width, with_right),
            grid=(tiles,),
            out_shape=tuple(out_shape),
            in_specs=[
                smem,
                smem,
                whole((all_rows, wide)),
                whole((all_rows, 3 * width)),
                whole((width, width)),
                whole((out_rows, 1)),
                pl.BlockSpec((all_rows, tile_cols), lambda j: (0, j)),
                pl.BlockSpec((all_rows, tile_cols), lambda j: (0, tiles - 1 - j)),
            ],
            out_specs=tuple(out_specs),
            scratch_shapes=[pltpu.VMEM((2 * width, all_rows), jnp.bfloat16)],
            compiler_params=pltpu.CompilerParams(
                dimension_semantics=("arbitrary",), vmem_limit_bytes=60 * 2**20
            ),
            cost_estimate=pl.CostEstimate(
                flops=4 * width * all_rows * width_all,
                bytes_accessed=4 * all_rows * width_all,
                transcendentals=0,
            ),
            name="fold",
        )(
            mission_weight,
            span,
            proj_all,
            picked_all,
            jnp.asarray(perm, jnp.bfloat16),
            row_ids,
            design_all,
            design_all,
        )

    def ring(dm, dy):
        pairs = []
        for m in range(groups):
            for a in range(members):
                o, y, c = a // (inner * mid), (a // inner) % mid, a % inner
                target = (o * mid + (y + dy) % mid) * inner + c
                pairs.append((m * members + a, (m + dm) % groups * members + target))
        return pairs

    right = None
    folds, vectors = [], []
    for first in range(0, len(shifts), per_call):
        here = shifts[first : first + per_call]
        owners = [
            (group + dm) % groups * members + member_of((mid_at + dy) % mid) for dm, dy in here
        ]
        fold, tail, *extra = fold_call(owners, right is None)
        if right is None:
            right = extra[0][0]
        for at, (dm, dy) in enumerate(here):
            rows = slice(at * final_rows, (at + 1) * final_rows)
            block = fold[rows]
            vector = jnp.concatenate(
                [
                    lax.dynamic_slice_in_dim(right, owners[at] * right_cols, right_cols),
                    tail[0, rows],
                ]
            )
            if dm or dy:
                block = lax.ppermute(block, ("mission", "arc"), ring(dm, dy))
                vector = lax.ppermute(vector, ("mission", "arc"), ring(dm, dy))
            folds.append(block.astype(jnp.float32))
            vectors.append(vector)
    fold_total = functools.reduce(jnp.add, folds)
    vector_total = functools.reduce(jnp.add, vectors)
    return (fold_total, vector_total[:right_cols], vector_total[right_cols:])


TILES = 8
ARRIVAL = (0, 2, 7, 5, 6, 4, 3, 1)
Y_FIRST = (True, True, True, True, True, False, True, False)
SWAPPED = tuple(ARRIVAL.index(tile ^ 1) for tile in ARRIVAL)


def tile_at(slot, half):
    tile = ARRIVAL[slot]
    return tile + half * (1 - 2 * (tile % 2))


def scoped(step):
    @functools.wraps(step)
    def run(*at):
        with jax.named_scope("_".join([step.__name__, *map(str, at[:1])])):
            return step(*at)

    return run


def slot_of(tile, half):
    return ARRIVAL.index(tile ^ half)


def flip_matrix(size):
    return (
        (
            lax.broadcasted_iota(jnp.int32, (size, size), 0)
            + lax.broadcasted_iota(jnp.int32, (size, size), 1)
            == size - 1
        )
        .astype(jnp.float32)
        .astype(jnp.bfloat16)
    )


def in_line(ref, wide, fill):
    line = ref[...].reshape(1, -1)
    return jnp.concatenate([line, jnp.full((1, wide - line.shape[1]), fill, line.dtype)], axis=1)


def projector_start(sizes_ref, kinds_ref, nuis_ref, arc_ref, kind_ref):
    rows = nuis_ref.shape[0]
    wide = rounded_up(rows + 1, LANES)
    lane = lax.broadcasted_iota(jnp.int32, (rows, wide), 1)
    sub = lax.broadcasted_iota(jnp.int32, (rows, wide), 0)
    arc_row = in_line(arc_ref, wide, -1).astype(jnp.float32)
    kind_row = in_line(kind_ref, wide, -1)
    scale_row = jnp.ones((1, wide), jnp.float32)
    for kind in range(kinds_ref.shape[0]):
        scale_row = jnp.where(kind_row == kind, 1.0 / kinds_ref[kind], scale_row)
    arc_col = jnp.sum(jnp.where(lane == sub, arc_row, 0.0), axis=1, keepdims=True)
    size = jnp.zeros((rows, 1), jnp.int32)
    for arc in range(sizes_ref.shape[0]):
        size = jnp.where(arc_col == arc, sizes_ref[arc], size)
    nuis = nuis_ref[...].astype(jnp.float32)
    nuis = jnp.where(lax.broadcasted_iota(jnp.int32, nuis.shape, 1) < size, nuis, 0.0)
    padded = jnp.concatenate(
        [nuis, jnp.zeros((wide - rows, nuis.shape[1]), jnp.float32)], axis=0
    )
    gram = lax.dot_general(
        nuis.astype(jnp.bfloat16),
        padded.astype(jnp.bfloat16),
        (((1,), (1,)), ((), ())),
        preferred_element_type=jnp.float32,
    )
    state = jnp.where(arc_col == arc_row, gram, 0.0)
    return state + jnp.where(lane == sub, scale_row, 0.0)


def eliminate(state, first, last):
    rows, wide = state.shape
    deep = 8
    lane = lax.broadcasted_iota(jnp.int32, (deep, wide), 1)
    sub = lax.broadcasted_iota(jnp.int32, (deep, wide), 0)
    bands = [state[at : at + deep] for at in range(0, rows, deep)]
    for k in range(first, last):
        at, off = k // deep, k % deep
        row = bands[at][off : off + 1, :]
        inv = 1.0 / row[:, k : k + 1]
        scaled = jnp.where(lane[:1] == k, inv, row * inv)
        for band in range(at, rows // deep):
            col = bands[band][:, k : k + 1]
            hit = lane == k
            if band == at:
                if off == deep - 1:
                    continue
                col = jnp.where(sub[:, :1] > off, col, 0.0)
                hit = hit & (sub > off)
            bands[band] = jnp.where(hit, 0.0, bands[band]) - col * scaled
    return jnp.concatenate(bands, axis=0)


def projector_end(state, weight_ref, obs_ref):
    rows = state.shape[0]
    lane = lax.broadcasted_iota(jnp.int32, state.shape, 1)
    sub = lax.broadcasted_iota(jnp.int32, state.shape, 0)
    pivot = jnp.sum(jnp.where(lane == sub, state, 0.0), axis=1, keepdims=True)
    factor = jnp.where(lane < sub, state, jnp.where(lane == sub, 1.0, 0.0))
    inverse = lax.dot_general(
        factor,
        factor * (weight_ref[0] / pivot),
        (((0,), (0,)), ((), ())),
        precision=lax.Precision.HIGHEST,
        preferred_element_type=jnp.float32,
    )[:rows]
    reduced_obs = jnp.sum(
        jnp.where(lane < rows, inverse * in_line(obs_ref, lane.shape[1], 0), 0.0), axis=1, keepdims=True
    )
    return jnp.where(lane == rows, reduced_obs, inverse).astype(jnp.bfloat16)


def normals_kernel(
    sizes_ref, kinds_ref, weight_ref, design_ref, nuis_ref, arc_ref, kind_ref, obs_ref,
    kept_ref, sent_ref, right_ref, tail_ref,
    gath, proj, state_ref, turned, lhs, right_lhs, part, first_in, second_out, second_in, vec, vec_in,
    own_sem, z_send, z_recv, x_send, x_recv, r_send, r_recv, d_send, d_recv,
    one_send, one_recv, two_send, two_recv, v_send, v_recv,
):
    rows = nuis_ref.shape[0]
    tile_cols = gath.shape[2]
    mission = lax.axis_index("mission")
    arc = lax.axis_index("arc")
    core = lax.rem(arc, 2)
    y = lax.rem(lax.div(arc, 2), 2)
    near = lax.rem(lax.div(arc, 4), 2)
    half = lax.div(arc, 8)
    group = 2 * mission + half

    def device(x=None, zh=None, zl=None, yy=None, c=None):
        x = mission if x is None else x
        zh = half if zh is None else zh
        zl = near if zl is None else zl
        yy = y if yy is None else yy
        c = core if c is None else c
        return (x, ((zh * 2 + zl) * 2 + yy) * 2 + c)

    x_peer = device(x=1 - mission)
    z_peer = device(zh=1 - half)
    sibling = device(c=1 - core)
    y_peer = device(yy=1 - y)
    near_peer = device(zl=1 - near)
    cross_peer = device(zl=1 - near, yy=1 - y)

    def block(slot, at):
        span = pl.ds(at * rows, rows)
        return proj.at[span] if slot == TILES else gath.at[slot, span]

    def remote(src, dst, send, recv, target):
        return pltpu.make_async_remote_copy(
            src_ref=src,
            dst_ref=dst,
            send_sem=send,
            recv_sem=recv,
            device_id=target,
            device_id_type=pl.DeviceIdType.MESH,
        )

    def z_copy(slot):
        source = slot if slot == TILES else SWAPPED[slot]
        return remote(block(source, 0), block(slot, 2), z_send.at[slot], z_recv.at[slot], z_peer)

    def x_copy(slot):
        return remote(block(slot, 0), block(slot, 4), x_send.at[slot], x_recv.at[slot], x_peer)

    def relay(slot):
        return remote(block(slot, 2), block(slot, 6), r_send.at[slot], r_recv.at[slot], x_peer)

    def share(chip, slot):
        return remote(
            block(slot, 2 * chip),
            block(slot, 2 * chip + 1),
            d_send.at[chip, slot],
            d_recv.at[chip, slot],
            sibling,
        )

    def own_copy(slot):
        start = tile_at(slot, half) * tile_cols
        return pltpu.make_async_copy(
            design_ref.at[:, pl.ds(pl.multiple_of(start, LANES), tile_cols)],
            block(slot, 0),
            own_sem.at[slot],
        )

    def stage_one(n):
        if Y_FIRST[n]:
            src, target = part.at[n, :, 1 - y], y_peer
        else:
            src, target = part.at[n, 1 - near], near_peer
        return remote(src, first_in.at[n], one_send.at[n], one_recv.at[n], target)

    def stage_two(n):
        target = near_peer if Y_FIRST[n] else y_peer
        return remote(
            second_out.at[n], second_in.at[n], two_send.at[n], two_recv.at[n], target
        )

    def held(n, mine):
        if Y_FIRST[n]:
            at = near if mine else 1 - near
            return part[n, at, y].astype(jnp.float32) + first_in[n, at].astype(jnp.float32)
        at = y if mine else 1 - y
        return part[n, near, at].astype(jnp.float32) + first_in[n, at].astype(jnp.float32)

    def vector_copy(k):
        target = (y_peer, near_peer, cross_peer)[k]
        to = (2 * near + 1 - y, 2 * (1 - near) + y, 2 * (1 - near) + 1 - y)[k]
        return remote(vec.at[to], vec_in.at[k], v_send.at[k], v_recv.at[k], target)

    for slot in range(TILES):
        own_copy(slot).start()
    barrier = pltpu.get_barrier_semaphore()
    peers = (x_peer, z_peer, sibling, y_peer, near_peer, cross_peer)
    for peer in peers:
        pl.semaphore_signal(barrier, inc=1, device_id=peer, device_id_type=pl.DeviceIdType.MESH)
    step = rows // 16
    ends = near == half

    def apart(work):
        pl.when(arc >= 0)(work)

    def sweep(first, last):
        @apart
        def _():
            with jax.named_scope('elim'):
                state_ref[...] = eliminate(state_ref[...], first, last)

    @apart
    def _():
        state = projector_start(sizes_ref, kinds_ref, nuis_ref, arc_ref, kind_ref)
        state_ref[...] = eliminate(state, 0, 2 * step)

    pl.semaphore_wait(barrier, len(peers))
    for slot in range(TILES):
        own_copy(slot).wait()
    @scoped
    def from_z(slot):
        z_copy(slot).wait_recv()
        relay(slot).start()
        share(1, slot).start()

    @scoped
    def from_x(slot):
        x_copy(slot).wait_recv()
        share(2, slot).start()

    @scoped
    def from_relay(slot):
        relay(slot).wait_recv()
        share(3, slot).start()

    @scoped
    def settled(slot):
        for chip in range(4):
            share(chip, slot).wait_recv()

    def solved(slot):
        return jnp.concatenate(
            [
                jnp.dot(
                    proj[pl.ds(at * rows, rows), :][:, :rows],
                    gath[slot, pl.ds(at * rows, rows), :],
                    preferred_element_type=jnp.float32,
                )
                for at in range(2 * 4)
            ],
            axis=0,
        )

    @scoped
    def make_lhs(mirrored):
        turned[...] = solved(mission + 2 * mirrored).T.astype(jnp.bfloat16)
        for to in range(4):
            start = 2 * rows * to + rows * core
            if mirrored:
                start = tile_cols - rows - start
            picked = turned[pl.ds(pl.multiple_of(start, 16), rows), :]
            if mirrored:
                picked = jnp.dot(
                    flip_matrix(rows), picked, preferred_element_type=jnp.float32
                ).astype(jnp.bfloat16)
            lhs[mirrored, pl.ds(to * rows, rows), :] = picked

    def product(mirrored, slot):
        out = jnp.dot(lhs[mirrored], gath[slot], preferred_element_type=jnp.float32)
        if not mirrored:
            return out
        flip = flip_matrix(LANES)
        out = out.astype(jnp.bfloat16)
        return jnp.concatenate(
            [
                jnp.dot(out[:, start : start + LANES], flip, preferred_element_type=jnp.float32)
                for start in range(tile_cols - LANES, -1, -LANES)
            ],
            axis=1,
        )

    def put(n, value):
        part[n] = value.astype(jnp.bfloat16).reshape(2, 2, rows, tile_cols)

    def diagonal(n):
        local = lax.broadcasted_iota(jnp.int32, (4 * rows, tile_cols), 0)
        local = lax.div(local, rows) * (2 * rows) + lax.rem(local, rows) + rows * core
        cols = lax.broadcasted_iota(jnp.int32, (4 * rows, tile_cols), 1)
        put(n, jnp.where(cols >= local, product(0, mission), product(1, 2 + mission)))
        stage_one(n).start()

    def above(n, slot):
        put(n, product(0, slot))
        stage_one(n).start()

    def mirrored(n, slot):
        put(n, product(1, slot))
        stage_one(n).start()

    def low(work):
        pl.when(mission == 0)(work)

    def high(work):
        pl.when(mission == 1)(work)

    def on(x, zh):
        return pl.when(jnp.logical_and(mission == x, half == zh))

    @scoped
    def jobs_at(slot):
        if slot == 1:

            @low
            def _():
                above(0, 1)

        elif slot == 2:

            @low
            def _():
                above(1, 2)
                make_lhs(1)
                diagonal(2)

            @high
            def _():
                above(0, 2)

        elif slot == 3:

            @low
            def _():
                above(3, 3)

            @high
            def _():
                above(1, 3)
                make_lhs(1)
                diagonal(2)
                mirrored(3, 2)

        elif slot == 4:
            above(4, 4)

            @high
            def _():
                mirrored(5, 4)

            @on(0, 1)
            def _():
                mirrored(7, 4)

        elif slot == 5:

            @low
            def _():
                above(5, 5)

            @high
            def _():
                above(6, 5)

            @on(1, 1)
            def _():
                mirrored(7, 5)

        elif slot == 6:

            @low
            def _():
                above(6, 6)

            @on(1, 0)
            def _():
                above(7, 6)

        else:

            @on(0, 0)
            def _():
                above(7, 7)

    def out_tile(n):
        def upper(slot):
            return tile_at(slot, half)

        def lower(slot):
            return TILES - 1 - tile_at(slot, half)

        def by_mission(low, high):
            return low + mission * (high - low)

        return (
            lambda: by_mission(upper(1), upper(2)),
            lambda: by_mission(upper(2), upper(3)),
            lambda: group,
            lambda: by_mission(upper(3), lower(2)),
            lambda: upper(4),
            lambda: by_mission(upper(5), lower(4)),
            lambda: by_mission(upper(6), upper(5)),
            lambda: by_mission(
                upper(7) + half * (lower(4) - upper(7)),
                upper(6) + half * (lower(5) - upper(6)),
            ),
        )[n]()

    @scoped
    def pass_on(n):
        stage_one(n).wait_recv()
        second_out[n] = held(n, False).astype(jnp.bfloat16)
        stage_two(n).start()

    @scoped
    def finish(n):
        stage_two(n).wait_recv()
        start = pl.multiple_of(out_tile(n) * tile_cols, LANES)
        kept_ref[:, pl.ds(start, tile_cols)] = held(n, True).astype(jnp.bfloat16)
        sent_ref[:, pl.ds(start, tile_cols)] = second_in[n]

    @scoped
    def vectors():
        def by_place(a, b, c, d):
            return (1 - half) * (a + mission * (b - a)) + half * (c + mission * (d - c))

        low = by_place(
            slot_of(0, 0), slot_of(4, 0), slot_of(2, 1), slot_of(6, 1)
        )
        high = by_place(
            slot_of(1, 0), slot_of(5, 0), slot_of(3, 1), slot_of(7, 1)
        )
        last = by_place(
            slot_of(4, 0), slot_of(6, 0), slot_of(5, 1), slot_of(7, 1)
        )
        lines = [
            jnp.dot(right_lhs[...], gath[slot], preferred_element_type=jnp.float32)[:1]
            for slot in (low, high)
        ]
        reduced = solved(last).astype(jnp.bfloat16).astype(jnp.float32)
        lines.append(
            jnp.sum(gath[last].astype(jnp.float32) * reduced, axis=0, keepdims=True)
        )
        right = jnp.concatenate(lines[:2], axis=1)
        for to in range(4):
            parts = []
            for line, width in ((right, 2 * rows), (lines[2], rows)):
                even, odd = (
                    line[:, at * width : (at + 1) * width] for at in (2 * to, 2 * to + 1)
                )
                parts.append(jnp.where(core == 0, even, odd))
            parts.append(jnp.zeros((1, vec.shape[2] - 3 * rows), jnp.float32))
            vec[to, :1, :] = jnp.concatenate(parts, axis=1)
        for k in range(3):
            vector_copy(k).start()

    @scoped
    def next_z(slot):
        z_copy(slot).wait_send()
        if slot + 2 < TILES:

            @pl.when(jnp.logical_not(ends))
            def _():
                z_copy(slot + 2).start()

        early = (2,) if slot == 1 else (3, 4) if slot == 2 else (slot + 2,)
        early = tuple(at for at in early if 2 <= at < TILES) if slot else ()
        if early:

            @pl.when(ends)
            def _():
                for at in early:
                    z_copy(at).start()

    def next_x(slot):
        x_copy(slot).start()

    z_copy(0).start()
    x_copy(0).start()
    z_copy(1).start()
    x_copy(1).start()
    x_copy(2).start()
    for slot in range(TILES):
        share(0, slot).start()
    sweep(2 * step, rows)

    @apart
    @scoped
    def project():
        proj[pl.ds(0, rows), :] = projector_end(state_ref[...], weight_ref, obs_ref)

    z_copy(TILES).start()
    x_copy(TILES).start()
    share(0, TILES).start()
    from_x(0)
    from_x(1)
    from_z(0)
    next_z(0)
    from_x(TILES)
    from_z(1)
    next_x(3)
    next_z(1)
    from_relay(0)
    from_z(TILES)
    from_x(2)
    next_x(4)
    from_relay(1)
    settled(0)
    from_z(2)
    next_z(2)
    from_relay(TILES)
    settled(1)
    settled(TILES)
    make_lhs(0)
    jobs_at(1)
    right_lhs[...] = proj[...].astype(jnp.float32).T.astype(jnp.bfloat16)[rows : rows + 16]
    from_x(3)
    from_relay(2)
    from_z(3)
    next_z(3)
    next_x(5)
    settled(2)
    jobs_at(2)
    from_x(4)
    from_relay(3)
    from_z(4)
    next_z(4)
    next_x(6)
    settled(3)
    jobs_at(3)
    pass_on(0)
    from_x(5)
    from_relay(4)
    from_z(5)
    next_z(5)
    next_x(7)
    settled(4)
    jobs_at(4)
    pass_on(1)
    from_x(6)
    from_relay(5)
    from_z(6)
    next_z(6)
    settled(5)
    jobs_at(5)
    pass_on(2)
    pass_on(3)
    finish(0)
    from_x(7)
    from_relay(6)
    from_z(7)
    next_z(7)
    settled(6)
    jobs_at(6)
    pass_on(4)
    finish(1)
    from_relay(7)
    settled(7)
    jobs_at(7)
    vectors()
    pass_on(5)
    finish(2)
    finish(3)
    pass_on(6)
    finish(4)
    finish(5)
    pass_on(7)
    finish(6)
    total = vec[2 * near + y, :1, :]
    for k in range(3):
        vector_copy(k).wait_recv()
        total = total + vec_in[k, :1, :]
    right_ref[...] = total[:, : 2 * rows]
    tail_ref[...] = total[:, 2 * rows : 3 * rows]
    finish(7)

    z_copy(TILES).wait_send()
    for slot in range(TILES + 1):
        x_copy(slot).wait_send()
        relay(slot).wait_send()
        for chip in range(4):
            share(chip, slot).wait_send()
    for n in range(TILES):
        stage_one(n).wait_send()
        stage_two(n).wait_send()
    for k in range(3):
        vector_copy(k).wait_send()


def on_paired_chips(
    design,
    nuisance_design,
    observed,
    arc_of_row,
    nuis_size,
    weight_index,
    kind_weight,
    mission_weight,
):
    rows, width_all = design.shape
    wide = rounded_up(rows + 1, LANES)
    tile_cols = width_all // TILES
    stacked = 2 * 4 * rows
    vec_cols = rounded_up(3 * rows, LANES)
    vmem = pl.BlockSpec(memory_space=pltpu.VMEM)
    smem = pl.BlockSpec(memory_space=pltpu.SMEM)
    dma = pltpu.SemaphoreType.DMA
    slots = TILES + 1

    kept, sent, right, tail = pl.pallas_call(
        normals_kernel,
        out_shape=(
            jax.ShapeDtypeStruct((rows, width_all), jnp.bfloat16),
            jax.ShapeDtypeStruct((rows, width_all), jnp.bfloat16),
            jax.ShapeDtypeStruct((1, 2 * rows), jnp.float32),
            jax.ShapeDtypeStruct((1, rows), jnp.float32),
        ),
        in_specs=[smem, smem, smem, pl.BlockSpec(memory_space=pl.ANY), vmem, vmem, vmem, vmem],
        out_specs=(vmem, vmem, vmem, vmem),
        scratch_shapes=[
            pltpu.VMEM((TILES, stacked, tile_cols), jnp.bfloat16),
            pltpu.VMEM((stacked, wide), jnp.bfloat16),
            pltpu.VMEM((rows, wide), jnp.float32),
            pltpu.VMEM((tile_cols, stacked), jnp.bfloat16),
            pltpu.VMEM((2, 4 * rows, stacked), jnp.bfloat16),
            pltpu.VMEM((16, stacked), jnp.bfloat16),
            pltpu.VMEM((TILES, 2, 2, rows, tile_cols), jnp.bfloat16),
            pltpu.VMEM((TILES, 2, rows, tile_cols), jnp.bfloat16),
            pltpu.VMEM((TILES, rows, tile_cols), jnp.bfloat16),
            pltpu.VMEM((TILES, rows, tile_cols), jnp.bfloat16),
            pltpu.VMEM((4, 8, vec_cols), jnp.float32),
            pltpu.VMEM((3, 8, vec_cols), jnp.float32),
            dma((TILES,)),
            dma((slots,)),
            dma((slots,)),
            dma((slots,)),
            dma((slots,)),
            dma((slots,)),
            dma((slots,)),
            dma((4, slots)),
            dma((4, slots)),
            dma((TILES,)),
            dma((TILES,)),
            dma((TILES,)),
            dma((TILES,)),
            dma((3,)),
            dma((3,)),
        ],
        compiler_params=pltpu.CompilerParams(
            collective_id=0, has_side_effects=True, vmem_limit_bytes=60 * 2**20
        ),
        name="normals",
    )(
        nuis_size,
        kind_weight,
        mission_weight,
        design,
        nuisance_design,
        arc_of_row,
        weight_index,
        observed,
    )
    fold = kept.astype(jnp.float32) + sent.astype(jnp.float32)
    return fold, right.reshape(-1), tail.reshape(-1)


def solution(mesh):
    placed = (
        P(("mission", "arc"), None),
        P(("mission", "arc"), None),
        P(("mission", "arc")),
        P(("mission", "arc")),
        P(("mission", "arc")),
        P(("mission", "arc")),
        P(),
        P("mission"),
    )

    def on_device(design, *rest):
        devices = lax.axis_size("mission") * lax.axis_size("arc")
        paired = lax.axis_size("mission") == 2 and lax.axis_size("arc") == 16
        rows, width_all = design.shape
        if paired and width_all == 2 * devices * rows and rows % 16 == 0 and width_all % (TILES * LANES) == 0:
            return on_paired_chips(design, *rest)
        return on_any_mesh(design, *rest)

    return jax.shard_map(
        on_device,
        mesh=mesh,
        in_specs=placed,
        out_specs=(P(("mission", "arc"), None), P(("mission", "arc")), P(("mission", "arc"))),
        check_vma=False,
    )
```

```python
import functools

import jax
import jax.numpy as jnp
import numpy as np
from jax import lax
from jax.experimental import pallas as pl
from jax.experimental.pallas import tpu as pltpu
from jax.sharding import PartitionSpec as P

LANES = 128


def rounded_up(value, unit):
    return -(-value // unit) * unit


def projector_kernel(
    sizes_ref, kinds_ref, nuis_ref, arc_col_ref, arc_row_ref, kind_col_ref, obs_row_ref, out_ref
):
    rows, wide = out_ref.shape
    arc_col = arc_col_ref[...]
    kind_col = kind_col_ref[...]
    weight = jnp.zeros((rows, 1), jnp.float32)
    for kind in range(kinds_ref.shape[0]):
        weight = jnp.where(kind_col == kind, kinds_ref[kind], weight)
    size = jnp.zeros((rows, 1), jnp.int32)
    for arc in range(sizes_ref.shape[0]):
        size = jnp.where(arc_col == arc, sizes_ref[arc], size)
    nuis = nuis_ref[...].astype(jnp.float32)
    nuis = jnp.where(lax.broadcasted_iota(jnp.int32, nuis.shape, 1) < size, nuis, 0.0)
    padded = jnp.concatenate(
        [nuis, jnp.zeros((wide - rows, nuis.shape[1]), jnp.float32)], axis=0
    )
    gram = lax.dot_general(
        nuis.astype(jnp.bfloat16),
        padded.astype(jnp.bfloat16),
        (((1,), (1,)), ((), ())),
        preferred_element_type=jnp.float32,
    )
    lane = lax.broadcasted_iota(jnp.int32, (rows, wide), 1)
    sub = lax.broadcasted_iota(jnp.int32, (rows, wide), 0)
    state = jnp.where(arc_col == arc_row_ref[...], gram, 0.0)
    state = state + jnp.where(lane == sub, 1.0 / weight, 0.0)
    for k in range(rows):
        row = state[k : k + 1, :]
        col = state[:, k : k + 1]
        inv = 1.0 / row[:, k : k + 1]
        scaled_row = row * inv
        scaled_col = col * inv
        swept = state - col * scaled_row
        swept = jnp.where(lane == k, scaled_col, swept)
        swept = jnp.where(sub == k, scaled_row, swept)
        state = jnp.where((lane == k) & (sub == k), -inv, swept)
    inverse = -state
    reduced_obs = jnp.sum(inverse * obs_row_ref[...], axis=1, keepdims=True)
    out_ref[...] = jnp.where(lane == rows, reduced_obs, inverse).astype(out_ref.dtype)


def fold_kernel(
    block_rows,
    width,
    with_right,
    weight_ref,
    span_ref,
    proj_ref,
    picked_ref,
    perm_ref,
    rows_ref,
    above_ref,
    mirror_ref,
    fold_ref,
    tail_ref,
    *rest,
):
    lhs_ref = rest[-1]
    tile = pl.program_id(0)
    tile_cols = above_ref.shape[1]
    out_rows = fold_ref.shape[0]
    weight = weight_ref[0]

    @pl.when(tile == 0)
    def _():
        tail = jnp.zeros((1, width), jnp.float32)
        lane = lax.broadcasted_iota(jnp.int32, (block_rows, width), 1)
        pieces = []
        for block in range(proj_ref.shape[0] // block_rows):
            span = pl.ds(block * block_rows, block_rows)
            proj = proj_ref[span, :]
            picked = picked_ref[span, :]
            reduced = lax.dot_general(
                proj[:, :block_rows], picked, (((1,), (0,)), ((), ())),
                preferred_element_type=jnp.float32,
            )
            tail_reduced = reduced[:, 2 * width :].astype(jnp.bfloat16).astype(jnp.float32)
            tail += jnp.sum(
                picked[:, 2 * width :].astype(jnp.float32) * tail_reduced, axis=0, keepdims=True
            )
            first = jnp.where(
                lane == width - 1,
                proj[:, block_rows : block_rows + 1].astype(jnp.float32),
                reduced[:, :width],
            )
            second = jnp.dot(
                reduced[:, width : 2 * width].astype(jnp.bfloat16),
                perm_ref[...],
                preferred_element_type=jnp.float32,
            )
            pieces.append(jnp.concatenate([first, second], axis=1))
        lhs_ref[...] = jnp.concatenate(pieces, axis=0).T.astype(jnp.bfloat16)
        tail_ref[...] = weight * tail

    low, high = span_ref[0], span_ref[1]
    col_start = tile * tile_cols
    all_above = col_start >= high
    all_mirror = col_start + tile_cols <= low

    def above_tile():
        return weight * jnp.dot(
            lhs_ref[pl.ds(0, width), :], above_ref[...], preferred_element_type=jnp.float32
        )

    def mirror_tile():
        mirror = jnp.dot(
            lhs_ref[pl.ds(width, rounded_up(out_rows, 16)), :],
            mirror_ref[...],
            preferred_element_type=jnp.float32,
        )[:out_rows]
        mirror = (weight * mirror).astype(jnp.bfloat16)
        flip = (
            lax.broadcasted_iota(jnp.int32, (LANES, LANES), 0)
            + lax.broadcasted_iota(jnp.int32, (LANES, LANES), 1)
            == LANES - 1
        ).astype(jnp.float32).astype(jnp.bfloat16)
        return jnp.concatenate(
            [
                jnp.dot(
                    mirror[:, start : start + LANES], flip, preferred_element_type=jnp.float32
                )
                for start in range(tile_cols - LANES, -1, -LANES)
            ],
            axis=1,
        )

    if with_right:
        above = above_tile()
        rest[0][...] = above[width - 1 : width, :]
        fold_ref[...] = above[:out_rows].astype(fold_ref.dtype)
    else:

        @pl.when(jnp.logical_not(all_mirror))
        def _():
            fold_ref[...] = above_tile()[:out_rows].astype(fold_ref.dtype)

    @pl.when(all_mirror)
    def _():
        fold_ref[...] = mirror_tile().astype(fold_ref.dtype)

    @pl.when(jnp.logical_not(jnp.logical_or(all_above, all_mirror)))
    def _():
        cols = lax.broadcasted_iota(jnp.int32, (out_rows, tile_cols), 1) + col_start
        fold_ref[...] = jnp.where(
            cols >= rows_ref[...], fold_ref[...].astype(jnp.float32), mirror_tile()
        ).astype(fold_ref.dtype)


def on_any_mesh(
    design,
    nuisance_design,
    observed,
    arc_of_row,
    nuis_size,
    weight_index,
    kind_weight,
    mission_weight,
):
    groups = lax.axis_size("mission")
    members = lax.axis_size("arc")
    group = lax.axis_index("mission")
    member = lax.axis_index("arc")
    block_rows, width_all = design.shape
    half_width = width_all // 2
    final_rows = half_width // (groups * members)
    wide = rounded_up(block_rows + 1, LANES)
    inner = 2 if members % 2 == 0 else 1
    outer = 4 if members % (4 * inner) == 0 else 1
    mid = members // (outer * inner)
    mid_at = (member // inner) % mid
    gather_groups = [
        [(o * mid + y) * inner + c for o in range(outer) for c in range(inner)]
        for y in range(mid)
    ]

    def gathered(array):
        return lax.all_gather(
            array, "arc", axis=0, tiled=True, axis_index_groups=gather_groups
        )

    def member_of(y):
        return (member // (inner * mid) * mid + y) * inner + member % inner

    vmem = pl.BlockSpec(memory_space=pltpu.VMEM)
    smem = pl.BlockSpec(memory_space=pltpu.SMEM)

    design_all = gathered(design)

    proj = pl.pallas_call(
        projector_kernel,
        out_shape=jax.ShapeDtypeStruct((block_rows, wide), jnp.bfloat16),
        in_specs=[smem, smem, vmem, vmem, vmem, vmem, vmem],
        out_specs=vmem,
        cost_estimate=pl.CostEstimate(flops=10_000_000, bytes_accessed=100_000, transcendentals=0),
        name="projector",
    )(
        nuis_size,
        kind_weight,
        nuisance_design,
        arc_of_row[:, None],
        jnp.pad(arc_of_row, (0, wide - block_rows), constant_values=-1)[None, :],
        weight_index[:, None],
        jnp.pad(observed, (0, wide - block_rows))[None, :],
    )
    proj_all = gathered(proj)

    shifts = [(dm, dy) for dm in range(groups) for dy in range(mid)]
    shifts.sort(key=lambda shift: (shift[0] == 0, shift[1] == 0))
    per_call = max(1, len(shifts) // 2)
    out_rows = per_call * final_rows
    width = rounded_up(out_rows + 1, LANES)
    place = np.arange(out_rows)
    perm = np.zeros((width, width), np.float32)
    perm[(place // final_rows) * final_rows + final_rows - 1 - place % final_rows, place] = 1.0
    tile_cols = 512
    tiles = width_all // tile_cols
    all_rows = design_all.shape[0]
    right_cols = width_all // (groups * members)
    whole = lambda shape: pl.BlockSpec(shape, lambda j: (0, 0))

    def fold_call(owners, with_right):
        def picked(start_of):
            parts = [
                lax.dynamic_slice_in_dim(design_all, start_of(owner), final_rows, 1)
                for owner in owners
            ]
            blank = jnp.zeros((all_rows, width - out_rows), design_all.dtype)
            return parts + [blank]

        picked_all = jnp.concatenate(
            picked(lambda block: block * final_rows)
            + picked(lambda block: width_all - (block + 1) * final_rows)
            + picked(lambda block: half_width + block * final_rows),
            axis=1,
        )
        starts = jnp.stack(owners).astype(jnp.int32) * final_rows
        row_ids = (
            starts[:, None] + jnp.arange(final_rows, dtype=jnp.int32)[None, :]
        ).reshape(out_rows, 1)
        span = jnp.stack([jnp.min(starts), jnp.max(starts) + final_rows - 1])
        out_shape = [
            jax.ShapeDtypeStruct((out_rows, width_all), jnp.bfloat16),
            jax.ShapeDtypeStruct((1, width), jnp.float32),
        ]
        out_specs = [
            pl.BlockSpec((out_rows, tile_cols), lambda j: (0, j)),
            whole((1, width)),
        ]
        if with_right:
            out_shape.append(jax.ShapeDtypeStruct((1, width_all), jnp.float32))
            out_specs.append(pl.BlockSpec((1, tile_cols), lambda j: (0, j)))
        return pl.pallas_call(
            functools.partial(fold_kernel, block_rows, width, with_right),
            grid=(tiles,),
            out_shape=tuple(out_shape),
            in_specs=[
                smem,
                smem,
                whole((all_rows, wide)),
                whole((all_rows, 3 * width)),
                whole((width, width)),
                whole((out_rows, 1)),
                pl.BlockSpec((all_rows, tile_cols), lambda j: (0, j)),
                pl.BlockSpec((all_rows, tile_cols), lambda j: (0, tiles - 1 - j)),
            ],
            out_specs=tuple(out_specs),
            scratch_shapes=[pltpu.VMEM((2 * width, all_rows), jnp.bfloat16)],
            compiler_params=pltpu.CompilerParams(
                dimension_semantics=("arbitrary",), vmem_limit_bytes=60 * 2**20
            ),
            cost_estimate=pl.CostEstimate(
                flops=4 * width * all_rows * width_all,
                bytes_accessed=4 * all_rows * width_all,
                transcendentals=0,
            ),
            name="fold",
        )(
            mission_weight,
            span,
            proj_all,
            picked_all,
            jnp.asarray(perm, jnp.bfloat16),
            row_ids,
            design_all,
            design_all,
        )

    def ring(dm, dy):
        pairs = []
        for m in range(groups):
            for a in range(members):
                o, y, c = a // (inner * mid), (a // inner) % mid, a % inner
                target = (o * mid + (y + dy) % mid) * inner + c
                pairs.append((m * members + a, (m + dm) % groups * members + target))
        return pairs

    right = None
    folds, vectors = [], []
    for first in range(0, len(shifts), per_call):
        here = shifts[first : first + per_call]
        owners = [
            (group + dm) % groups * members + member_of((mid_at + dy) % mid) for dm, dy in here
        ]
        fold, tail, *extra = fold_call(owners, right is None)
        if right is None:
            right = extra[0][0]
        for at, (dm, dy) in enumerate(here):
            rows = slice(at * final_rows, (at + 1) * final_rows)
            block = fold[rows]
            vector = jnp.concatenate(
                [
                    lax.dynamic_slice_in_dim(right, owners[at] * right_cols, right_cols),
                    tail[0, rows],
                ]
            )
            if dm or dy:
                block = lax.ppermute(block, ("mission", "arc"), ring(dm, dy))
                vector = lax.ppermute(vector, ("mission", "arc"), ring(dm, dy))
            folds.append(block.astype(jnp.float32))
            vectors.append(vector)
    fold_total = functools.reduce(jnp.add, folds)
    vector_total = functools.reduce(jnp.add, vectors)
    return (fold_total, vector_total[:right_cols], vector_total[right_cols:])


TILES = 8
ARRIVAL = (0, 2, 5, 7, 6, 4, 3, 1)
Y_FIRST = (
    (True, False, True, False, True, True, False, True,),
    (True, False, True, False, True, True, False, True,),
)
STRAIGHT = ((), ())
SWAPPED = tuple(ARRIVAL.index(tile ^ 1) for tile in ARRIVAL)


def tile_at(slot, half):
    tile = ARRIVAL[slot]
    return tile + half * (1 - 2 * (tile % 2))


def scoped(step):
    @functools.wraps(step)
    def run(*at):
        with jax.named_scope("_".join([step.__name__, *map(str, at[:1])])):
            return step(*at)

    return run


def slot_of(tile, half):
    return ARRIVAL.index(tile ^ half)


def flip_matrix(size):
    return (
        (
            lax.broadcasted_iota(jnp.int32, (size, size), 0)
            + lax.broadcasted_iota(jnp.int32, (size, size), 1)
            == size - 1
        )
        .astype(jnp.float32)
        .astype(jnp.bfloat16)
    )


def in_line(ref, wide, fill):
    line = ref[...].reshape(1, -1)
    return jnp.concatenate([line, jnp.full((1, wide - line.shape[1]), fill, line.dtype)], axis=1)


def projector_start(sizes_ref, kinds_ref, nuis_ref, arc_ref, kind_ref):
    rows = nuis_ref.shape[0]
    wide = rounded_up(rows + 1, LANES)
    lane = lax.broadcasted_iota(jnp.int32, (rows, wide), 1)
    sub = lax.broadcasted_iota(jnp.int32, (rows, wide), 0)
    arc_row = in_line(arc_ref, wide, -1).astype(jnp.float32)
    kind_row = in_line(kind_ref, wide, -1)
    scale_row = jnp.ones((1, wide), jnp.float32)
    for kind in range(kinds_ref.shape[0]):
        scale_row = jnp.where(kind_row == kind, 1.0 / kinds_ref[kind], scale_row)
    arc_col = jnp.sum(jnp.where(lane == sub, arc_row, 0.0), axis=1, keepdims=True)
    size = jnp.zeros((rows, 1), jnp.int32)
    for arc in range(sizes_ref.shape[0]):
        size = jnp.where(arc_col == arc, sizes_ref[arc], size)
    nuis = nuis_ref[...].astype(jnp.float32)
    nuis = jnp.where(lax.broadcasted_iota(jnp.int32, nuis.shape, 1) < size, nuis, 0.0)
    padded = jnp.concatenate(
        [nuis, jnp.zeros((wide - rows, nuis.shape[1]), jnp.float32)], axis=0
    )
    gram = lax.dot_general(
        nuis.astype(jnp.bfloat16),
        padded.astype(jnp.bfloat16),
        (((1,), (1,)), ((), ())),
        preferred_element_type=jnp.float32,
    )
    state = jnp.where(arc_col == arc_row, gram, 0.0)
    return state + jnp.where(lane == sub, scale_row, 0.0)


def eliminate(state, first, last):
    rows, wide = state.shape
    deep = 8
    lane = lax.broadcasted_iota(jnp.int32, (deep, wide), 1)
    sub = lax.broadcasted_iota(jnp.int32, (deep, wide), 0)
    bands = [state[at : at + deep] for at in range(0, rows, deep)]
    for k in range(first, last):
        at, off = k // deep, k % deep
        row = bands[at][off : off + 1, :]
        inv = 1.0 / row[:, k : k + 1]
        scaled = jnp.where(lane[:1] == k, inv, row * inv)
        for band in range(at, rows // deep):
            col = bands[band][:, k : k + 1]
            hit = lane == k
            if band == at:
                if off == deep - 1:
                    continue
                col = jnp.where(sub[:, :1] > off, col, 0.0)
                hit = hit & (sub > off)
            bands[band] = jnp.where(hit, 0.0, bands[band]) - col * scaled
    return jnp.concatenate(bands, axis=0)


def projector_end(state, weight_ref, obs_ref):
    rows = state.shape[0]
    lane = lax.broadcasted_iota(jnp.int32, state.shape, 1)
    sub = lax.broadcasted_iota(jnp.int32, state.shape, 0)
    pivot = jnp.sum(jnp.where(lane == sub, state, 0.0), axis=1, keepdims=True)
    factor = jnp.where(lane < sub, state, jnp.where(lane == sub, 1.0, 0.0))
    inverse = lax.dot_general(
        factor,
        factor * (weight_ref[...].reshape(1, 1) / pivot),
        (((0,), (0,)), ((), ())),
        precision=lax.Precision.HIGHEST,
        preferred_element_type=jnp.float32,
    )[:rows]
    reduced_obs = jnp.sum(
        jnp.where(lane < rows, inverse * in_line(obs_ref, lane.shape[1], 0), 0.0), axis=1, keepdims=True
    )
    return jnp.where(lane == rows, reduced_obs, inverse).astype(jnp.bfloat16)


def normals_kernel(
    sizes_ref, kinds_ref, weight_ref, design_ref, nuis_ref, arc_ref, kind_ref, obs_ref,
    fold_ref, right_ref, tail_ref,
    gath, proj, state_ref, turned, lhs, right_lhs, part, first_in, second_out, second_in, vec, vec_in,
    own_sem, z_send, z_recv, x_send, x_recv, r_send, r_recv, d_send, d_recv,
    one_send, one_recv, two_send, two_recv, s_send, s_recv, v_send, v_recv,
):
    rows = nuis_ref.shape[0]
    tile_cols = gath.shape[2]
    mission = lax.axis_index("mission")
    arc = lax.axis_index("arc")
    core = lax.rem(arc, 2)
    y = lax.rem(lax.div(arc, 2), 2)
    near = lax.rem(lax.div(arc, 4), 2)
    half = lax.div(arc, 8)
    group = 2 * mission + half

    def device(x=None, zh=None, zl=None, yy=None, c=None):
        x = mission if x is None else x
        zh = half if zh is None else zh
        zl = near if zl is None else zl
        yy = y if yy is None else yy
        c = core if c is None else c
        return (x, ((zh * 2 + zl) * 2 + yy) * 2 + c)

    x_peer = device(x=1 - mission)
    z_peer = device(zh=1 - half)
    sibling = device(c=1 - core)
    y_peer = device(yy=1 - y)
    near_peer = device(zl=1 - near)
    cross_peer = device(zl=1 - near, yy=1 - y)

    def block(slot, at):
        span = pl.ds(at * rows, rows)
        return proj.at[span] if slot == TILES else gath.at[slot, span]

    def remote(src, dst, send, recv, target):
        return pltpu.make_async_remote_copy(
            src_ref=src,
            dst_ref=dst,
            send_sem=send,
            recv_sem=recv,
            device_id=target,
            device_id_type=pl.DeviceIdType.MESH,
        )

    def z_copy(slot):
        source = slot if slot == TILES else SWAPPED[slot]
        return remote(block(source, 0), block(slot, 2), z_send.at[slot], z_recv.at[slot], z_peer)

    def x_copy(slot):
        return remote(block(slot, 0), block(slot, 4), x_send.at[slot], x_recv.at[slot], x_peer)

    def relay(slot):
        return remote(block(slot, 2), block(slot, 6), r_send.at[slot], r_recv.at[slot], x_peer)

    def share(chip, slot):
        return remote(
            block(slot, 2 * chip),
            block(slot, 2 * chip + 1),
            d_send.at[chip, slot],
            d_recv.at[chip, slot],
            sibling,
        )

    def own_copy(slot):
        start = tile_at(slot, half) * tile_cols
        return pltpu.make_async_copy(
            design_ref.at[:, pl.ds(pl.multiple_of(start, LANES), tile_cols)],
            block(slot, 0),
            own_sem.at[slot],
        )

    for slot in range(TILES):
        own_copy(slot).start()
    barrier = pltpu.get_barrier_semaphore()
    peers = (x_peer, z_peer, sibling, y_peer, near_peer, cross_peer)
    for peer in peers:
        pl.semaphore_signal(barrier, inc=1, device_id=peer, device_id_type=pl.DeviceIdType.MESH)
    ends = near == half

    def apart(work):
        pl.when(arc >= 0)(work)

    @apart
    def _():
        state_ref[...] = projector_start(sizes_ref, kinds_ref, nuis_ref, arc_ref, kind_ref)

    pl.semaphore_wait(barrier, len(peers))
    for slot in range(TILES):
        own_copy(slot).wait()
    def run(side):
        y_first, straight_jobs = Y_FIRST[side], STRAIGHT[side]

        def stage_one(n, k):
            if y_first[n]:
                zl, yy, to, target = (near if k else 1 - near), 1 - y, (near if k else 1 - near), y_peer
            else:
                zl, yy, to, target = 1 - near, (y if k else 1 - y), (y if k else 1 - y), near_peer
            return remote(
                part.at[n, zl, yy], first_in.at[n, to], one_send.at[n, k], one_recv.at[n, k], target
            )

        def straight(n):
            picks = (
                (near, 1 - y, first_in.at[n, 0], y_peer),
                (1 - near, y, first_in.at[n, 1], near_peer),
                (1 - near, 1 - y, second_in.at[n], cross_peer),
            )
            at = straight_jobs.index(n)
            return [
                remote(part.at[n, zl, yy], dst, s_send.at[at, k], s_recv.at[at, k], target)
                for k, (zl, yy, dst, target) in enumerate(picks)
            ]

        def stage_two(n):
            target = near_peer if y_first[n] else y_peer
            return remote(
                second_out.at[n], second_in.at[n], two_send.at[n], two_recv.at[n], target
            )

        def held(n, mine):
            if y_first[n]:
                at = near if mine else 1 - near
                return part[n, at, y].astype(jnp.float32) + first_in[n, at].astype(jnp.float32)
            at = y if mine else 1 - y
            return part[n, near, at].astype(jnp.float32) + first_in[n, at].astype(jnp.float32)

        def vector_copy(k):
            target = (y_peer, near_peer, cross_peer)[k]
            to = (2 * near + 1 - y, 2 * (1 - near) + y, 2 * (1 - near) + 1 - y)[k]
            return remote(vec.at[to], vec_in.at[k], v_send.at[k], v_recv.at[k], target)

        first, last = 0, TILES - 1
        def when(condition, work):
            if condition is True:
                work()
            elif condition is not False:
                pl.when(condition)(work)

        def here(slot):
            return {first: side == 0, last: half == 0 if side == 0 else False}.get(slot, True)

        def at_x_peer(slot):
            return {first: side == 1, last: half == 0 if side == 1 else False}.get(slot, True)

        def to_z_peer(slot):
            return half == 1 if slot == last else True

        def by_z(slot):
            return half == 0 if slot == last else True

        def start_z(slot):
            when(to_z_peer(slot), lambda: z_copy(slot).start())

        def start_x(slot):
            when(at_x_peer(slot), lambda: x_copy(slot).start())

        def start_share(slot):
            when(here(slot), lambda: share(0, slot).start())

        def z_if(condition, slot):
            extra = to_z_peer(slot)
            both = condition if extra is True else jnp.logical_and(condition, extra)
            pl.when(both)(z_copy(slot).start)

        def z_end(slot):
            z_if(ends, slot)

        def z_mid(slot):
            z_if(jnp.logical_not(ends), slot)

        @scoped
        def from_z(slot):
            def pass_along():
                z_copy(slot).wait_recv()
                when(at_x_peer(slot), lambda: relay(slot).start())
                when(here(slot), lambda: share(1, slot).start())

            when(by_z(slot), pass_along)

        @scoped
        def from_x(slot):
            def pass_along():
                x_copy(slot).wait_recv()
                share(2, slot).start()

            when(here(slot), pass_along)

        @scoped
        def from_relay(slot):
            def pass_along():
                relay(slot).wait_recv()
                share(3, slot).start()

            when(here(slot), pass_along)

        @scoped
        def settled(slot):
            def wait():
                for chip in range(4):
                    share(chip, slot).wait_recv()

            when(here(slot), wait)

        def solved(slot):
            return jnp.concatenate(
                [
                    jnp.dot(
                        proj[pl.ds(at * rows, rows), :][:, :rows],
                        gath[slot, pl.ds(at * rows, rows), :],
                        preferred_element_type=jnp.float32,
                    )
                    for at in range(2 * 4)
                ],
                axis=0,
            )

        @scoped
        def make_lhs(mirrored):
            turned[...] = solved(side + (3 - 2 * side) * mirrored).T.astype(jnp.bfloat16)
            for to in range(4):
                start = 2 * rows * to + rows * core
                if mirrored:
                    start = tile_cols - rows - start
                picked = turned[pl.ds(pl.multiple_of(start, 16), rows), :]
                if mirrored:
                    picked = jnp.dot(
                        flip_matrix(rows), picked, preferred_element_type=jnp.float32
                    ).astype(jnp.bfloat16)
                lhs[mirrored, pl.ds(to * rows, rows), :] = picked

        def product(mirrored, slot):
            out = jnp.dot(lhs[mirrored], gath[slot], preferred_element_type=jnp.float32)
            if not mirrored:
                return out
            flip = flip_matrix(LANES)
            out = out.astype(jnp.bfloat16)
            return jnp.concatenate(
                [
                    jnp.dot(out[:, start : start + LANES], flip, preferred_element_type=jnp.float32)
                    for start in range(tile_cols - LANES, -1, -LANES)
                ],
                axis=1,
            )

        def put(n, value):
            part[n] = value.astype(jnp.bfloat16).reshape(2, 2, rows, tile_cols)

        def send_out(n):
            for copy in straight(n) if n in straight_jobs else [stage_one(n, 0), stage_one(n, 1)]:
                copy.start()

        def diagonal(n):
            local = lax.broadcasted_iota(jnp.int32, (4 * rows, tile_cols), 0)
            local = lax.div(local, rows) * (2 * rows) + lax.rem(local, rows) + rows * core
            cols = lax.broadcasted_iota(jnp.int32, (4 * rows, tile_cols), 1)
            put(n, jnp.where(cols >= local, product(0, side), product(1, 3 - side)))
            send_out(n)

        def above(n, slot):
            put(n, product(0, slot))
            send_out(n)

        def mirrored(n, slot):
            put(n, product(1, slot))
            send_out(n)

        def on_low(work):
            if side == 0:
                work()

        def on_high(work):
            if side == 1:
                work()

        def on(x, zh):
            return pl.when(half == zh) if side == x else lambda work: None

        @scoped
        def jobs_at(slot):
            if slot == 1:

                @on_low
                def _():
                    above(0, 1)

            elif slot == 2:

                @on_low
                def _():
                    above(1, 2)

                @on_high
                def _():
                    above(0, 2)
                    make_lhs(1)
                    diagonal(1)

            elif slot == 3:

                @on_low
                def _():
                    above(2, 3)
                    make_lhs(1)
                    diagonal(3)

                @on_high
                def _():
                    above(2, 3)
                    mirrored(3, 3)

            elif slot == 4:
                above(4, 4)

                @on_high
                def _():
                    mirrored(5, 4)

                @on(0, 1)
                def _():
                    mirrored(7, 4)

            elif slot == 5:

                @on_low
                def _():
                    above(5, 5)

                @on_high
                def _():
                    above(6, 5)

                @on(1, 1)
                def _():
                    mirrored(7, 5)

            elif slot == 6:

                @on_low
                def _():
                    above(6, 6)

                @on(1, 0)
                def _():
                    above(7, 6)

            else:

                @on(0, 0)
                def _():
                    above(7, 7)

        def out_tile(n):
            def upper(slot):
                return tile_at(slot, half)

            def lower(slot):
                return TILES - 1 - tile_at(slot, half)

            def by_mission(one, two):
                return two if side else one

            return (
                lambda: by_mission(upper(1), upper(2)),
                lambda: by_mission(upper(2), group),
                lambda: upper(3),
                lambda: by_mission(group, lower(3)),
                lambda: upper(4),
                lambda: by_mission(upper(5), lower(4)),
                lambda: by_mission(upper(6), upper(5)),
                lambda: by_mission(
                    upper(7) + half * (lower(4) - upper(7)),
                    upper(6) + half * (lower(5) - upper(6)),
                ),
            )[n]()

        @scoped
        def pass_on(n):
            stage_one(n, 0).wait_recv()
            second_out[n] = held(n, False).astype(jnp.bfloat16)
            stage_two(n).start()

        @scoped
        def finish(n):
            start = pl.multiple_of(out_tile(n) * tile_cols, LANES)
            if n in straight_jobs:
                for copy in straight(n):
                    copy.wait_recv()
                total = part[n, near, y].astype(jnp.float32)
                for block in (first_in[n, 0], first_in[n, 1], second_in[n]):
                    total = total + block.astype(jnp.float32)
                fold_ref[:, pl.ds(start, tile_cols)] = total
                return
            stage_one(n, 1).wait_recv()
            stage_two(n).wait_recv()
            fold_ref[:, pl.ds(start, tile_cols)] = held(n, True) + second_in[n].astype(jnp.float32)

        @scoped
        def vectors():
            def by_place(a, b, c, d):
                return (1 - half) * (b if side else a) + half * (d if side else c)

            low = by_place(
                slot_of(0, 0), slot_of(4, 0), slot_of(2, 1), slot_of(6, 1)
            )
            high = by_place(
                slot_of(1, 0), slot_of(5, 0), slot_of(3, 1), slot_of(7, 1)
            )
            last = by_place(
                slot_of(4, 0), slot_of(6, 0), slot_of(5, 1), slot_of(7, 1)
            )
            lines = [
                jnp.dot(right_lhs[...], gath[slot], preferred_element_type=jnp.float32)[:1]
                for slot in (low, high)
            ]
            reduced = solved(last).astype(jnp.bfloat16).astype(jnp.float32)
            lines.append(
                jnp.sum(gath[last].astype(jnp.float32) * reduced, axis=0, keepdims=True)
            )
            right = jnp.concatenate(lines[:2], axis=1)
            for to in range(4):
                parts = []
                for line, width in ((right, 2 * rows), (lines[2], rows)):
                    even, odd = (
                        line[:, at * width : (at + 1) * width] for at in (2 * to, 2 * to + 1)
                    )
                    parts.append(jnp.where(core == 0, even, odd))
                parts.append(jnp.zeros((1, vec.shape[2] - 3 * rows), jnp.float32))
                vec[to, :1, :] = jnp.concatenate(parts, axis=1)
            for k in range(3):
                vector_copy(k).start()

        def sweep(start, stop):
            @apart
            def _():
                state_ref[...] = eliminate(state_ref[...], start, stop)

        @scoped
        def project():
            @apart
            def _():
                proj[pl.ds(0, rows), :] = projector_end(state_ref[...], weight_ref, obs_ref)

            z_copy(TILES).start()
            x_copy(TILES).start()
            share(0, TILES).start()

        def gather_sent():
            for slot in range(TILES + 1):
                when(to_z_peer(slot), lambda: z_copy(slot).wait_send())
                when(at_x_peer(slot), lambda: x_copy(slot).wait_send())
                when(at_x_peer(slot), lambda: relay(slot).wait_send())
                for chip in range(4):
                    when(here(slot), lambda: share(chip, slot).wait_send())

        def sum_sent(n):
            for copy in straight(n) if n in straight_jobs else [stage_one(n, 0), stage_one(n, 1), stage_two(n)]:
                copy.wait_send()

        def right_side_row():
            turned_rows = proj[...].astype(jnp.float32).T.astype(jnp.bfloat16)
            right_lhs[...] = turned_rows[rows : rows + 16]

        def add_vectors():
            total = vec[2 * near + y, :1, :]
            for k in range(3):
                vector_copy(k).wait_recv()
                total = total + vec_in[k, :1, :]
            right_ref[...] = total[:, : 2 * rows]
            tail_ref[...] = total[:, 2 * rows : 3 * rows]


        if side == 0:
            start_share(0)
            start_x(0)
            start_z(0)
            start_z(1)
            start_x(1)
            start_x(4)
            start_x(2)
            sweep(0 * rows // 80, 16 * rows // 80)
            sweep(16 * rows // 80, 32 * rows // 80)
            start_share(3)
            start_share(1)
            sweep(32 * rows // 80, 48 * rows // 80)
            sweep(48 * rows // 80, 64 * rows // 80)
            sweep(64 * rows // 80, 80 * rows // 80)
            from_x(0)
            project()
            z_mid(2)
            from_x(TILES)
            z_end(2)
            from_z(0)
            z_mid(3)
            start_x(3)
            start_share(4)
            from_x(1)
            from_z(TILES)
            from_relay(0)
            z_mid(4)
            from_x(4)
            from_z(1)
            from_relay(TILES)
            z_mid(7)
            z_mid(5)
            start_share(2)
            z_end(3)
            from_z(2)
            from_relay(1)
            settled(TILES)
            right_side_row()
            from_x(2)
            start_x(5)
            from_relay(2)
            settled(1)
            z_end(4)
            from_x(3)
            start_share(7)
            settled(0)
            z_mid(6)
            make_lhs(0)
            z_end(7)
            jobs_at(1)
            from_z(3)
            settled(2)
            jobs_at(2)
            from_z(4)
            from_relay(3)
            start_x(6)
            start_x(7)
            from_x(5)
            start_share(6)
            z_end(5)
            z_end(6)
            settled(3)
            jobs_at(3)
            from_relay(4)
            settled(4)
            jobs_at(4)
            from_x(7)
            from_z(5)
            pass_on(2)
            from_z(7)
            from_x(6)
            pass_on(4)
            pass_on(0)
            from_relay(5)
            pass_on(1)
            from_z(6)
            start_share(5)
            pass_on(3)
            from_relay(7)
            settled(5)
            settled(7)
            jobs_at(5)
            from_relay(6)
            settled(6)
            jobs_at(6)
            jobs_at(7)
            pass_on(6)
            pass_on(5)
            finish(4)
            finish(1)
            vectors()
            pass_on(7)
            finish(2)
            finish(5)
            finish(6)
            gather_sent()
            sum_sent(4)
            sum_sent(1)
            sum_sent(2)
            sum_sent(5)
            sum_sent(6)
            finish(3)
            finish(0)
            add_vectors()
            finish(7)
            sum_sent(3)
            sum_sent(0)
            sum_sent(7)
            for k in range(3):
                vector_copy(k).wait_send()
        else:
            start_share(0)
            start_x(0)
            start_z(0)
            start_z(1)
            start_x(1)
            start_x(4)
            start_x(2)
            sweep(0 * rows // 80, 16 * rows // 80)
            sweep(16 * rows // 80, 32 * rows // 80)
            start_share(3)
            start_share(1)
            sweep(32 * rows // 80, 48 * rows // 80)
            sweep(48 * rows // 80, 64 * rows // 80)
            sweep(64 * rows // 80, 80 * rows // 80)
            from_x(0)
            project()
            z_mid(2)
            from_x(TILES)
            z_end(2)
            from_z(0)
            z_mid(3)
            start_x(3)
            start_share(4)
            from_x(1)
            from_z(TILES)
            from_relay(0)
            z_mid(4)
            from_x(4)
            from_z(1)
            from_relay(TILES)
            z_mid(7)
            z_mid(5)
            start_share(2)
            z_end(3)
            from_z(2)
            from_relay(1)
            settled(TILES)
            right_side_row()
            from_x(2)
            start_x(5)
            from_relay(2)
            settled(1)
            z_end(4)
            from_x(3)
            start_share(7)
            settled(0)
            z_mid(6)
            make_lhs(0)
            z_end(7)
            jobs_at(1)
            from_z(3)
            settled(2)
            jobs_at(2)
            from_z(4)
            from_relay(3)
            start_x(6)
            start_x(7)
            from_x(5)
            start_share(6)
            z_end(5)
            z_end(6)
            settled(3)
            jobs_at(3)
            from_relay(4)
            settled(4)
            jobs_at(4)
            from_x(7)
            from_z(5)
            pass_on(2)
            from_z(7)
            from_x(6)
            pass_on(4)
            pass_on(0)
            from_relay(5)
            pass_on(1)
            from_z(6)
            start_share(5)
            pass_on(3)
            from_relay(7)
            settled(5)
            settled(7)
            jobs_at(5)
            from_relay(6)
            settled(6)
            jobs_at(6)
            jobs_at(7)
            pass_on(6)
            pass_on(5)
            finish(4)
            finish(1)
            vectors()
            pass_on(7)
            finish(2)
            finish(5)
            finish(6)
            gather_sent()
            sum_sent(4)
            sum_sent(1)
            sum_sent(2)
            sum_sent(5)
            sum_sent(6)
            finish(3)
            finish(0)
            add_vectors()
            finish(7)
            sum_sent(3)
            sum_sent(0)
            sum_sent(7)
            for k in range(3):
                vector_copy(k).wait_send()

    @pl.when(mission == 0)
    def _():
        run(0)

    @pl.when(mission == 1)
    def _():
        run(1)

def on_paired_chips(
    design,
    nuisance_design,
    observed,
    arc_of_row,
    nuis_size,
    weight_index,
    kind_weight,
    mission_weight,
):
    rows, width_all = design.shape
    wide = rounded_up(rows + 1, LANES)
    tile_cols = width_all // TILES
    stacked = 2 * 4 * rows
    vec_cols = rounded_up(3 * rows, LANES)
    vmem = pl.BlockSpec(memory_space=pltpu.VMEM)
    smem = pl.BlockSpec(memory_space=pltpu.SMEM)
    dma = pltpu.SemaphoreType.DMA
    slots = TILES + 1

    fold, right, tail = pl.pallas_call(
        normals_kernel,
        out_shape=(
            pltpu.VMEM((rows, width_all), jnp.float32),
            pltpu.VMEM((1, 2 * rows), jnp.float32),
            pltpu.VMEM((1, rows), jnp.float32),
        ),
        in_specs=[smem, smem, vmem, pl.BlockSpec(memory_space=pl.ANY), vmem, vmem, vmem, vmem],
        out_specs=(vmem, vmem, vmem),
        scratch_shapes=[
            pltpu.VMEM((TILES, stacked, tile_cols), jnp.bfloat16),
            pltpu.VMEM((stacked, wide), jnp.bfloat16),
            pltpu.VMEM((rows, wide), jnp.float32),
            pltpu.VMEM((tile_cols, stacked), jnp.bfloat16),
            pltpu.VMEM((2, 4 * rows, stacked), jnp.bfloat16),
            pltpu.VMEM((16, stacked), jnp.bfloat16),
            pltpu.VMEM((TILES, 2, 2, rows, tile_cols), jnp.bfloat16),
            pltpu.VMEM((TILES, 2, rows, tile_cols), jnp.bfloat16),
            pltpu.VMEM((TILES, rows, tile_cols), jnp.bfloat16),
            pltpu.VMEM((TILES, rows, tile_cols), jnp.bfloat16),
            pltpu.VMEM((4, 8, vec_cols), jnp.float32),
            pltpu.VMEM((3, 8, vec_cols), jnp.float32),
            dma((TILES,)),
            dma((slots,)),
            dma((slots,)),
            dma((slots,)),
            dma((slots,)),
            dma((slots,)),
            dma((slots,)),
            dma((4, slots)),
            dma((4, slots)),
            dma((TILES, 2)),
            dma((TILES, 2)),
            dma((TILES,)),
            dma((TILES,)),
            dma((1, 3)),
            dma((1, 3)),
            dma((3,)),
            dma((3,)),
        ],
        compiler_params=pltpu.CompilerParams(
            collective_id=0, has_side_effects=True, vmem_limit_bytes=60 * 2**20
        ),
        name="normals",
    )(
        nuis_size,
        kind_weight,
        mission_weight,
        design,
        nuisance_design,
        arc_of_row,
        weight_index,
        observed,
    )
    return fold, right.reshape(-1), tail.reshape(-1)


def solution(mesh):
    placed = (
        P(("mission", "arc"), None),
        P(("mission", "arc"), None),
        P(("mission", "arc")),
        P(("mission", "arc")),
        P(("mission", "arc")),
        P(("mission", "arc")),
        P(),
        P("mission"),
    )

    def on_device(design, *rest):
        devices = lax.axis_size("mission") * lax.axis_size("arc")
        paired = lax.axis_size("mission") == 2 and lax.axis_size("arc") == 16
        rows, width_all = design.shape
        if paired and width_all == 2 * devices * rows and rows % 16 == 0 and width_all % (TILES * LANES) == 0:
            return on_paired_chips(design, *rest)
        return on_any_mesh(design, *rest)

    return jax.shard_map(
        on_device,
        mesh=mesh,
        in_specs=placed,
        out_specs=(P(("mission", "arc"), None), P(("mission", "arc")), P(("mission", "arc"))),
        check_vma=False,
    )
```

```python
import functools

import jax
import jax.numpy as jnp
import numpy as np
from jax import lax
from jax.experimental import pallas as pl
from jax.experimental.pallas import tpu as pltpu
from jax.sharding import PartitionSpec as P

LANES = 128


def rounded_up(value, unit):
    return -(-value // unit) * unit


def projector_kernel(
    sizes_ref, kinds_ref, nuis_ref, arc_col_ref, arc_row_ref, kind_col_ref, obs_row_ref, out_ref
):
    rows, wide = out_ref.shape
    arc_col = arc_col_ref[...]
    kind_col = kind_col_ref[...]
    weight = jnp.zeros((rows, 1), jnp.float32)
    for kind in range(kinds_ref.shape[0]):
        weight = jnp.where(kind_col == kind, kinds_ref[kind], weight)
    size = jnp.zeros((rows, 1), jnp.int32)
    for arc in range(sizes_ref.shape[0]):
        size = jnp.where(arc_col == arc, sizes_ref[arc], size)
    nuis = nuis_ref[...].astype(jnp.float32)
    nuis = jnp.where(lax.broadcasted_iota(jnp.int32, nuis.shape, 1) < size, nuis, 0.0)
    padded = jnp.concatenate(
        [nuis, jnp.zeros((wide - rows, nuis.shape[1]), jnp.float32)], axis=0
    )
    gram = lax.dot_general(
        nuis.astype(jnp.bfloat16),
        padded.astype(jnp.bfloat16),
        (((1,), (1,)), ((), ())),
        preferred_element_type=jnp.float32,
    )
    lane = lax.broadcasted_iota(jnp.int32, (rows, wide), 1)
    sub = lax.broadcasted_iota(jnp.int32, (rows, wide), 0)
    state = jnp.where(arc_col == arc_row_ref[...], gram, 0.0)
    state = state + jnp.where(lane == sub, 1.0 / weight, 0.0)
    for k in range(rows):
        row = state[k : k + 1, :]
        col = state[:, k : k + 1]
        inv = 1.0 / row[:, k : k + 1]
        scaled_row = row * inv
        scaled_col = col * inv
        swept = state - col * scaled_row
        swept = jnp.where(lane == k, scaled_col, swept)
        swept = jnp.where(sub == k, scaled_row, swept)
        state = jnp.where((lane == k) & (sub == k), -inv, swept)
    inverse = -state
    reduced_obs = jnp.sum(inverse * obs_row_ref[...], axis=1, keepdims=True)
    out_ref[...] = jnp.where(lane == rows, reduced_obs, inverse).astype(out_ref.dtype)


def fold_kernel(
    block_rows,
    width,
    with_right,
    weight_ref,
    span_ref,
    proj_ref,
    picked_ref,
    perm_ref,
    rows_ref,
    above_ref,
    mirror_ref,
    fold_ref,
    tail_ref,
    *rest,
):
    lhs_ref = rest[-1]
    tile = pl.program_id(0)
    tile_cols = above_ref.shape[1]
    out_rows = fold_ref.shape[0]
    weight = weight_ref[0]

    @pl.when(tile == 0)
    def _():
        tail = jnp.zeros((1, width), jnp.float32)
        lane = lax.broadcasted_iota(jnp.int32, (block_rows, width), 1)
        pieces = []
        for block in range(proj_ref.shape[0] // block_rows):
            span = pl.ds(block * block_rows, block_rows)
            proj = proj_ref[span, :]
            picked = picked_ref[span, :]
            reduced = lax.dot_general(
                proj[:, :block_rows], picked, (((1,), (0,)), ((), ())),
                preferred_element_type=jnp.float32,
            )
            tail_reduced = reduced[:, 2 * width :].astype(jnp.bfloat16).astype(jnp.float32)
            tail += jnp.sum(
                picked[:, 2 * width :].astype(jnp.float32) * tail_reduced, axis=0, keepdims=True
            )
            first = jnp.where(
                lane == width - 1,
                proj[:, block_rows : block_rows + 1].astype(jnp.float32),
                reduced[:, :width],
            )
            second = jnp.dot(
                reduced[:, width : 2 * width].astype(jnp.bfloat16),
                perm_ref[...],
                preferred_element_type=jnp.float32,
            )
            pieces.append(jnp.concatenate([first, second], axis=1))
        lhs_ref[...] = jnp.concatenate(pieces, axis=0).T.astype(jnp.bfloat16)
        tail_ref[...] = weight * tail

    low, high = span_ref[0], span_ref[1]
    col_start = tile * tile_cols
    all_above = col_start >= high
    all_mirror = col_start + tile_cols <= low

    def above_tile():
        return weight * jnp.dot(
            lhs_ref[pl.ds(0, width), :], above_ref[...], preferred_element_type=jnp.float32
        )

    def mirror_tile():
        mirror = jnp.dot(
            lhs_ref[pl.ds(width, rounded_up(out_rows, 16)), :],
            mirror_ref[...],
            preferred_element_type=jnp.float32,
        )[:out_rows]
        mirror = (weight * mirror).astype(jnp.bfloat16)
        flip = (
            lax.broadcasted_iota(jnp.int32, (LANES, LANES), 0)
            + lax.broadcasted_iota(jnp.int32, (LANES, LANES), 1)
            == LANES - 1
        ).astype(jnp.float32).astype(jnp.bfloat16)
        return jnp.concatenate(
            [
                jnp.dot(
                    mirror[:, start : start + LANES], flip, preferred_element_type=jnp.float32
                )
                for start in range(tile_cols - LANES, -1, -LANES)
            ],
            axis=1,
        )

    if with_right:
        above = above_tile()
        rest[0][...] = above[width - 1 : width, :]
        fold_ref[...] = above[:out_rows].astype(fold_ref.dtype)
    else:

        @pl.when(jnp.logical_not(all_mirror))
        def _():
            fold_ref[...] = above_tile()[:out_rows].astype(fold_ref.dtype)

    @pl.when(all_mirror)
    def _():
        fold_ref[...] = mirror_tile().astype(fold_ref.dtype)

    @pl.when(jnp.logical_not(jnp.logical_or(all_above, all_mirror)))
    def _():
        cols = lax.broadcasted_iota(jnp.int32, (out_rows, tile_cols), 1) + col_start
        fold_ref[...] = jnp.where(
            cols >= rows_ref[...], fold_ref[...].astype(jnp.float32), mirror_tile()
        ).astype(fold_ref.dtype)


def on_any_mesh(
    design,
    nuisance_design,
    observed,
    arc_of_row,
    nuis_size,
    weight_index,
    kind_weight,
    mission_weight,
):
    groups = lax.axis_size("mission")
    members = lax.axis_size("arc")
    group = lax.axis_index("mission")
    member = lax.axis_index("arc")
    block_rows, width_all = design.shape
    half_width = width_all // 2
    final_rows = half_width // (groups * members)
    wide = rounded_up(block_rows + 1, LANES)
    inner = 2 if members % 2 == 0 else 1
    outer = 4 if members % (4 * inner) == 0 else 1
    mid = members // (outer * inner)
    mid_at = (member // inner) % mid
    gather_groups = [
        [(o * mid + y) * inner + c for o in range(outer) for c in range(inner)]
        for y in range(mid)
    ]

    def gathered(array):
        return lax.all_gather(
            array, "arc", axis=0, tiled=True, axis_index_groups=gather_groups
        )

    def member_of(y):
        return (member // (inner * mid) * mid + y) * inner + member % inner

    vmem = pl.BlockSpec(memory_space=pltpu.VMEM)
    smem = pl.BlockSpec(memory_space=pltpu.SMEM)

    design_all = gathered(design)

    proj = pl.pallas_call(
        projector_kernel,
        out_shape=jax.ShapeDtypeStruct((block_rows, wide), jnp.bfloat16),
        in_specs=[smem, smem, vmem, vmem, vmem, vmem, vmem],
        out_specs=vmem,
        cost_estimate=pl.CostEstimate(flops=10_000_000, bytes_accessed=100_000, transcendentals=0),
        name="projector",
    )(
        nuis_size,
        kind_weight,
        nuisance_design,
        arc_of_row[:, None],
        jnp.pad(arc_of_row, (0, wide - block_rows), constant_values=-1)[None, :],
        weight_index[:, None],
        jnp.pad(observed, (0, wide - block_rows))[None, :],
    )
    proj_all = gathered(proj)

    shifts = [(dm, dy) for dm in range(groups) for dy in range(mid)]
    shifts.sort(key=lambda shift: (shift[0] == 0, shift[1] == 0))
    per_call = max(1, len(shifts) // 2)
    out_rows = per_call * final_rows
    width = rounded_up(out_rows + 1, LANES)
    place = np.arange(out_rows)
    perm = np.zeros((width, width), np.float32)
    perm[(place // final_rows) * final_rows + final_rows - 1 - place % final_rows, place] = 1.0
    tile_cols = 512
    tiles = width_all // tile_cols
    all_rows = design_all.shape[0]
    right_cols = width_all // (groups * members)
    whole = lambda shape: pl.BlockSpec(shape, lambda j: (0, 0))

    def fold_call(owners, with_right):
        def picked(start_of):
            parts = [
                lax.dynamic_slice_in_dim(design_all, start_of(owner), final_rows, 1)
                for owner in owners
            ]
            blank = jnp.zeros((all_rows, width - out_rows), design_all.dtype)
            return parts + [blank]

        picked_all = jnp.concatenate(
            picked(lambda block: block * final_rows)
            + picked(lambda block: width_all - (block + 1) * final_rows)
            + picked(lambda block: half_width + block * final_rows),
            axis=1,
        )
        starts = jnp.stack(owners).astype(jnp.int32) * final_rows
        row_ids = (
            starts[:, None] + jnp.arange(final_rows, dtype=jnp.int32)[None, :]
        ).reshape(out_rows, 1)
        span = jnp.stack([jnp.min(starts), jnp.max(starts) + final_rows - 1])
        out_shape = [
            jax.ShapeDtypeStruct((out_rows, width_all), jnp.bfloat16),
            jax.ShapeDtypeStruct((1, width), jnp.float32),
        ]
        out_specs = [
            pl.BlockSpec((out_rows, tile_cols), lambda j: (0, j)),
            whole((1, width)),
        ]
        if with_right:
            out_shape.append(jax.ShapeDtypeStruct((1, width_all), jnp.float32))
            out_specs.append(pl.BlockSpec((1, tile_cols), lambda j: (0, j)))
        return pl.pallas_call(
            functools.partial(fold_kernel, block_rows, width, with_right),
            grid=(tiles,),
            out_shape=tuple(out_shape),
            in_specs=[
                smem,
                smem,
                whole((all_rows, wide)),
                whole((all_rows, 3 * width)),
                whole((width, width)),
                whole((out_rows, 1)),
                pl.BlockSpec((all_rows, tile_cols), lambda j: (0, j)),
                pl.BlockSpec((all_rows, tile_cols), lambda j: (0, tiles - 1 - j)),
            ],
            out_specs=tuple(out_specs),
            scratch_shapes=[pltpu.VMEM((2 * width, all_rows), jnp.bfloat16)],
            compiler_params=pltpu.CompilerParams(
                dimension_semantics=("arbitrary",), vmem_limit_bytes=60 * 2**20
            ),
            cost_estimate=pl.CostEstimate(
                flops=4 * width * all_rows * width_all,
                bytes_accessed=4 * all_rows * width_all,
                transcendentals=0,
            ),
            name="fold",
        )(
            mission_weight,
            span,
            proj_all,
            picked_all,
            jnp.asarray(perm, jnp.bfloat16),
            row_ids,
            design_all,
            design_all,
        )

    def ring(dm, dy):
        pairs = []
        for m in range(groups):
            for a in range(members):
                o, y, c = a // (inner * mid), (a // inner) % mid, a % inner
                target = (o * mid + (y + dy) % mid) * inner + c
                pairs.append((m * members + a, (m + dm) % groups * members + target))
        return pairs

    right = None
    folds, vectors = [], []
    for first in range(0, len(shifts), per_call):
        here = shifts[first : first + per_call]
        owners = [
            (group + dm) % groups * members + member_of((mid_at + dy) % mid) for dm, dy in here
        ]
        fold, tail, *extra = fold_call(owners, right is None)
        if right is None:
            right = extra[0][0]
        for at, (dm, dy) in enumerate(here):
            rows = slice(at * final_rows, (at + 1) * final_rows)
            block = fold[rows]
            vector = jnp.concatenate(
                [
                    lax.dynamic_slice_in_dim(right, owners[at] * right_cols, right_cols),
                    tail[0, rows],
                ]
            )
            if dm or dy:
                block = lax.ppermute(block, ("mission", "arc"), ring(dm, dy))
                vector = lax.ppermute(vector, ("mission", "arc"), ring(dm, dy))
            folds.append(block.astype(jnp.float32))
            vectors.append(vector)
    fold_total = functools.reduce(jnp.add, folds)
    vector_total = functools.reduce(jnp.add, vectors)
    return (fold_total, vector_total[:right_cols], vector_total[right_cols:])


TILES = 8
ARRIVAL = (0, 2, 5, 7, 6, 4, 3, 1)
Y_FIRST = (
    (True, False, True, True, True, False, True, False,),
    (True, False, True, True, True, False, True, False,),
)
STRAIGHT = ((), ())
SWAPPED = tuple(ARRIVAL.index(tile ^ 1) for tile in ARRIVAL)


def tile_at(slot, half):
    tile = ARRIVAL[slot]
    return tile + half * (1 - 2 * (tile % 2))


def scoped(step):
    @functools.wraps(step)
    def run(*at):
        with jax.named_scope("_".join([step.__name__, *map(str, at[:1])])):
            return step(*at)

    return run


def slot_of(tile, half):
    return ARRIVAL.index(tile ^ half)


def flip_matrix(size):
    return (
        (
            lax.broadcasted_iota(jnp.int32, (size, size), 0)
            + lax.broadcasted_iota(jnp.int32, (size, size), 1)
            == size - 1
        )
        .astype(jnp.float32)
        .astype(jnp.bfloat16)
    )


def in_line(ref, wide, fill):
    line = ref[...].reshape(1, -1)
    return jnp.concatenate([line, jnp.full((1, wide - line.shape[1]), fill, line.dtype)], axis=1)


def projector_start(sizes_ref, kinds_ref, nuis_ref, arc_ref, kind_ref):
    rows = nuis_ref.shape[0]
    wide = rounded_up(rows + 1, LANES)
    lane = lax.broadcasted_iota(jnp.int32, (rows, wide), 1)
    sub = lax.broadcasted_iota(jnp.int32, (rows, wide), 0)
    arc_row = in_line(arc_ref, wide, -1).astype(jnp.float32)
    kind_row = in_line(kind_ref, wide, -1)
    scale_row = jnp.ones((1, wide), jnp.float32)
    for kind in range(kinds_ref.shape[0]):
        scale_row = jnp.where(kind_row == kind, 1.0 / kinds_ref[kind], scale_row)
    arc_col = jnp.sum(jnp.where(lane == sub, arc_row, 0.0), axis=1, keepdims=True)
    size = jnp.zeros((rows, 1), jnp.int32)
    for arc in range(sizes_ref.shape[0]):
        size = jnp.where(arc_col == arc, sizes_ref[arc], size)
    nuis = nuis_ref[...].astype(jnp.float32)
    nuis = jnp.where(lax.broadcasted_iota(jnp.int32, nuis.shape, 1) < size, nuis, 0.0)
    padded = jnp.concatenate(
        [nuis, jnp.zeros((wide - rows, nuis.shape[1]), jnp.float32)], axis=0
    )
    gram = lax.dot_general(
        nuis.astype(jnp.bfloat16),
        padded.astype(jnp.bfloat16),
        (((1,), (1,)), ((), ())),
        preferred_element_type=jnp.float32,
    )
    state = jnp.where(arc_col == arc_row, gram, 0.0)
    return state + jnp.where(lane == sub, scale_row, 0.0)


def eliminate(state, first, last):
    rows, wide = state.shape
    deep = 8
    lane = lax.broadcasted_iota(jnp.int32, (deep, wide), 1)
    sub = lax.broadcasted_iota(jnp.int32, (deep, wide), 0)
    bands = [state[at : at + deep] for at in range(0, rows, deep)]
    for k in range(first, last):
        at, off = k // deep, k % deep
        row = bands[at][off : off + 1, :]
        inv = 1.0 / row[:, k : k + 1]
        scaled = jnp.where(lane[:1] == k, inv, row * inv)
        for band in range(at, rows // deep):
            col = bands[band][:, k : k + 1]
            hit = lane == k
            if band == at:
                if off == deep - 1:
                    continue
                col = jnp.where(sub[:, :1] > off, col, 0.0)
                hit = hit & (sub > off)
            bands[band] = jnp.where(hit, 0.0, bands[band]) - col * scaled
    return jnp.concatenate(bands, axis=0)


def projector_end(state, weight_ref, obs_ref):
    rows = state.shape[0]
    lane = lax.broadcasted_iota(jnp.int32, state.shape, 1)
    sub = lax.broadcasted_iota(jnp.int32, state.shape, 0)
    pivot = jnp.sum(jnp.where(lane == sub, state, 0.0), axis=1, keepdims=True)
    factor = jnp.where(lane < sub, state, jnp.where(lane == sub, 1.0, 0.0))
    inverse = lax.dot_general(
        factor,
        factor * (weight_ref[...].reshape(1, 1) / pivot),
        (((0,), (0,)), ((), ())),
        precision=lax.Precision.HIGHEST,
        preferred_element_type=jnp.float32,
    )[:rows]
    reduced_obs = jnp.sum(
        jnp.where(lane < rows, inverse * in_line(obs_ref, lane.shape[1], 0), 0.0), axis=1, keepdims=True
    )
    return jnp.where(lane == rows, reduced_obs, inverse).astype(jnp.bfloat16)


def normals_kernel(
    sizes_ref, kinds_ref, weight_ref, design_ref, nuis_ref, arc_ref, kind_ref, obs_ref,
    fold_ref, right_ref, tail_ref,
    gath, proj, state_ref, turned, lhs, right_lhs, part, first_in, second_out, second_in, vec, vec_in,
    own_sem, z_send, z_recv, x_send, x_recv, r_send, r_recv, d_send, d_recv,
    one_send, one_recv, two_send, two_recv, s_send, s_recv, v_send, v_recv,
):
    rows = nuis_ref.shape[0]
    tile_cols = gath.shape[2]
    mission = lax.axis_index("mission")
    arc = lax.axis_index("arc")
    core = lax.rem(arc, 2)
    y = lax.rem(lax.div(arc, 2), 2)
    near = lax.rem(lax.div(arc, 4), 2)
    half = lax.div(arc, 8)
    group = 2 * mission + half

    def device(x=None, zh=None, zl=None, yy=None, c=None):
        x = mission if x is None else x
        zh = half if zh is None else zh
        zl = near if zl is None else zl
        yy = y if yy is None else yy
        c = core if c is None else c
        return (x, ((zh * 2 + zl) * 2 + yy) * 2 + c)

    x_peer = device(x=1 - mission)
    z_peer = device(zh=1 - half)
    sibling = device(c=1 - core)
    y_peer = device(yy=1 - y)
    near_peer = device(zl=1 - near)
    cross_peer = device(zl=1 - near, yy=1 - y)

    def block(slot, at):
        span = pl.ds(at * rows, rows)
        return proj.at[span] if slot == TILES else gath.at[slot, span]

    def remote(src, dst, send, recv, target):
        return pltpu.make_async_remote_copy(
            src_ref=src,
            dst_ref=dst,
            send_sem=send,
            recv_sem=recv,
            device_id=target,
            device_id_type=pl.DeviceIdType.MESH,
        )

    def z_copy(slot):
        source = slot if slot == TILES else SWAPPED[slot]
        return remote(block(source, 0), block(slot, 2), z_send.at[slot], z_recv.at[slot], z_peer)

    def x_copy(slot):
        return remote(block(slot, 0), block(slot, 4), x_send.at[slot], x_recv.at[slot], x_peer)

    def relay(slot):
        return remote(block(slot, 2), block(slot, 6), r_send.at[slot], r_recv.at[slot], x_peer)

    def share(chip, slot):
        return remote(
            block(slot, 2 * chip),
            block(slot, 2 * chip + 1),
            d_send.at[chip, slot],
            d_recv.at[chip, slot],
            sibling,
        )

    def own_copy(slot):
        start = tile_at(slot, half) * tile_cols
        return pltpu.make_async_copy(
            design_ref.at[:, pl.ds(pl.multiple_of(start, LANES), tile_cols)],
            block(slot, 0),
            own_sem.at[slot],
        )

    for slot in range(TILES):
        own_copy(slot).start()
    barrier = pltpu.get_barrier_semaphore()
    peers = (x_peer, z_peer, sibling, y_peer, near_peer, cross_peer)
    for peer in peers:
        pl.semaphore_signal(barrier, inc=1, device_id=peer, device_id_type=pl.DeviceIdType.MESH)
    ends = near == half

    def apart(work):
        pl.when(arc >= 0)(work)

    @apart
    def _():
        state_ref[...] = projector_start(sizes_ref, kinds_ref, nuis_ref, arc_ref, kind_ref)

    pl.semaphore_wait(barrier, len(peers))
    for slot in range(TILES):
        own_copy(slot).wait()
    def run(side):
        y_first, straight_jobs = Y_FIRST[side], STRAIGHT[side]

        def stage_one(n, k):
            if y_first[n]:
                zl, yy, to, target = (near if k else 1 - near), 1 - y, (near if k else 1 - near), y_peer
            else:
                zl, yy, to, target = 1 - near, (y if k else 1 - y), (y if k else 1 - y), near_peer
            return remote(
                part.at[n, zl, yy], first_in.at[n, to], one_send.at[n, k], one_recv.at[n, k], target
            )

        def straight(n):
            picks = (
                (near, 1 - y, first_in.at[n, 0], y_peer),
                (1 - near, y, first_in.at[n, 1], near_peer),
                (1 - near, 1 - y, second_in.at[n], cross_peer),
            )
            at = straight_jobs.index(n)
            return [
                remote(part.at[n, zl, yy], dst, s_send.at[at, k], s_recv.at[at, k], target)
                for k, (zl, yy, dst, target) in enumerate(picks)
            ]

        def stage_two(n):
            target = near_peer if y_first[n] else y_peer
            return remote(
                second_out.at[n], second_in.at[n], two_send.at[n], two_recv.at[n], target
            )

        def held(n, mine):
            if y_first[n]:
                at = near if mine else 1 - near
                return part[n, at, y].astype(jnp.float32) + first_in[n, at].astype(jnp.float32)
            at = y if mine else 1 - y
            return part[n, near, at].astype(jnp.float32) + first_in[n, at].astype(jnp.float32)

        def vector_copy(k):
            target = (y_peer, near_peer, cross_peer)[k]
            to = (2 * near + 1 - y, 2 * (1 - near) + y, 2 * (1 - near) + 1 - y)[k]
            return remote(vec.at[to], vec_in.at[k], v_send.at[k], v_recv.at[k], target)

        first, last = 0, TILES - 1
        def when(condition, work):
            if condition is True:
                work()
            elif condition is not False:
                pl.when(condition)(work)

        def here(slot):
            return {first: side == 0, last: half == 0 if side == 0 else False}.get(slot, True)

        def at_x_peer(slot):
            return {first: side == 1, last: half == 0 if side == 1 else False}.get(slot, True)

        def to_z_peer(slot):
            return half == 1 if slot == last else True

        def by_z(slot):
            return half == 0 if slot == last else True

        def start_z(slot):
            when(to_z_peer(slot), lambda: z_copy(slot).start())

        def start_x(slot):
            when(at_x_peer(slot), lambda: x_copy(slot).start())

        def start_share(slot):
            when(here(slot), lambda: share(0, slot).start())

        def z_if(condition, slot):
            extra = to_z_peer(slot)
            both = condition if extra is True else jnp.logical_and(condition, extra)
            pl.when(both)(z_copy(slot).start)

        def z_end(slot):
            z_if(ends, slot)

        def z_mid(slot):
            z_if(jnp.logical_not(ends), slot)

        @scoped
        def from_z(slot):
            def pass_along():
                z_copy(slot).wait_recv()
                when(at_x_peer(slot), lambda: relay(slot).start())
                when(here(slot), lambda: share(1, slot).start())

            when(by_z(slot), pass_along)

        @scoped
        def from_x(slot):
            def pass_along():
                x_copy(slot).wait_recv()
                share(2, slot).start()

            when(here(slot), pass_along)

        @scoped
        def from_relay(slot):
            def pass_along():
                relay(slot).wait_recv()
                share(3, slot).start()

            when(here(slot), pass_along)

        @scoped
        def settled(slot):
            def wait():
                for chip in range(4):
                    share(chip, slot).wait_recv()

            when(here(slot), wait)

        def solved(slot):
            return jnp.concatenate(
                [
                    jnp.dot(
                        proj[pl.ds(at * rows, rows), :][:, :rows],
                        gath[slot, pl.ds(at * rows, rows), :],
                        preferred_element_type=jnp.float32,
                    )
                    for at in range(2 * 4)
                ],
                axis=0,
            )

        @scoped
        def make_lhs(mirrored):
            turned[...] = solved(side + (3 - 2 * side) * mirrored).T.astype(jnp.bfloat16)
            for to in range(4):
                start = 2 * rows * to + rows * core
                if mirrored:
                    start = tile_cols - rows - start
                picked = turned[pl.ds(pl.multiple_of(start, 16), rows), :]
                if mirrored:
                    picked = jnp.dot(
                        flip_matrix(rows), picked, preferred_element_type=jnp.float32
                    ).astype(jnp.bfloat16)
                lhs[mirrored, pl.ds(to * rows, rows), :] = picked

        def product(mirrored, slot):
            out = jnp.dot(lhs[mirrored], gath[slot], preferred_element_type=jnp.float32)
            if not mirrored:
                return out
            flip = flip_matrix(LANES)
            out = out.astype(jnp.bfloat16)
            return jnp.concatenate(
                [
                    jnp.dot(out[:, start : start + LANES], flip, preferred_element_type=jnp.float32)
                    for start in range(tile_cols - LANES, -1, -LANES)
                ],
                axis=1,
            )

        def put(n, value):
            part[n] = value.astype(jnp.bfloat16).reshape(2, 2, rows, tile_cols)

        def send_out(n):
            for copy in straight(n) if n in straight_jobs else [stage_one(n, 0), stage_one(n, 1)]:
                copy.start()

        def diagonal(n):
            local = lax.broadcasted_iota(jnp.int32, (4 * rows, tile_cols), 0)
            local = lax.div(local, rows) * (2 * rows) + lax.rem(local, rows) + rows * core
            cols = lax.broadcasted_iota(jnp.int32, (4 * rows, tile_cols), 1)
            put(n, jnp.where(cols >= local, product(0, side), product(1, 3 - side)))
            send_out(n)

        def above(n, slot):
            put(n, product(0, slot))
            send_out(n)

        def mirrored(n, slot):
            put(n, product(1, slot))
            send_out(n)

        def on_low(work):
            if side == 0:
                work()

        def on_high(work):
            if side == 1:
                work()

        def on(x, zh):
            return pl.when(half == zh) if side == x else lambda work: None

        @scoped
        def jobs_at(slot):
            if slot == 1:

                @on_low
                def _():
                    above(0, 1)

            elif slot == 2:

                @on_low
                def _():
                    above(1, 2)

                @on_high
                def _():
                    above(0, 2)
                    make_lhs(1)
                    diagonal(1)

            elif slot == 3:

                @on_low
                def _():
                    above(2, 3)
                    make_lhs(1)
                    diagonal(3)

                @on_high
                def _():
                    above(2, 3)
                    mirrored(3, 3)

            elif slot == 4:
                above(4, 4)

                @on_high
                def _():
                    mirrored(5, 4)

                @on(0, 1)
                def _():
                    mirrored(7, 4)

            elif slot == 5:

                @on_low
                def _():
                    above(5, 5)

                @on_high
                def _():
                    above(6, 5)

                @on(1, 1)
                def _():
                    mirrored(7, 5)

            elif slot == 6:

                @on_low
                def _():
                    above(6, 6)

                @on(1, 0)
                def _():
                    above(7, 6)

            else:

                @on(0, 0)
                def _():
                    above(7, 7)

        def out_tile(n):
            def upper(slot):
                return tile_at(slot, half)

            def lower(slot):
                return TILES - 1 - tile_at(slot, half)

            def by_mission(one, two):
                return two if side else one

            return (
                lambda: by_mission(upper(1), upper(2)),
                lambda: by_mission(upper(2), group),
                lambda: upper(3),
                lambda: by_mission(group, lower(3)),
                lambda: upper(4),
                lambda: by_mission(upper(5), lower(4)),
                lambda: by_mission(upper(6), upper(5)),
                lambda: by_mission(
                    upper(7) + half * (lower(4) - upper(7)),
                    upper(6) + half * (lower(5) - upper(6)),
                ),
            )[n]()

        @scoped
        def pass_on(n):
            stage_one(n, 0).wait_recv()
            second_out[n] = held(n, False).astype(jnp.bfloat16)
            stage_two(n).start()

        @scoped
        def finish(n):
            start = pl.multiple_of(out_tile(n) * tile_cols, LANES)
            if n in straight_jobs:
                for copy in straight(n):
                    copy.wait_recv()
                total = part[n, near, y].astype(jnp.float32)
                for block in (first_in[n, 0], first_in[n, 1], second_in[n]):
                    total = total + block.astype(jnp.float32)
                fold_ref[:, pl.ds(start, tile_cols)] = total
                return
            stage_one(n, 1).wait_recv()
            stage_two(n).wait_recv()
            fold_ref[:, pl.ds(start, tile_cols)] = held(n, True) + second_in[n].astype(jnp.float32)

        @scoped
        def vectors():
            def by_place(a, b, c, d):
                return (1 - half) * (b if side else a) + half * (d if side else c)

            low = by_place(
                slot_of(0, 0), slot_of(4, 0), slot_of(2, 1), slot_of(6, 1)
            )
            high = by_place(
                slot_of(1, 0), slot_of(5, 0), slot_of(3, 1), slot_of(7, 1)
            )
            last = by_place(
                slot_of(4, 0), slot_of(6, 0), slot_of(5, 1), slot_of(7, 1)
            )
            lines = [
                jnp.dot(right_lhs[...], gath[slot], preferred_element_type=jnp.float32)[:1]
                for slot in (low, high)
            ]
            reduced = solved(last).astype(jnp.bfloat16).astype(jnp.float32)
            lines.append(
                jnp.sum(gath[last].astype(jnp.float32) * reduced, axis=0, keepdims=True)
            )
            right = jnp.concatenate(lines[:2], axis=1)
            for to in range(4):
                parts = []
                for line, width in ((right, 2 * rows), (lines[2], rows)):
                    even, odd = (
                        line[:, at * width : (at + 1) * width] for at in (2 * to, 2 * to + 1)
                    )
                    parts.append(jnp.where(core == 0, even, odd))
                parts.append(jnp.zeros((1, vec.shape[2] - 3 * rows), jnp.float32))
                vec[to, :1, :] = jnp.concatenate(parts, axis=1)
            for k in range(3):
                vector_copy(k).start()

        def sweep(start, stop):
            @apart
            def _():
                state_ref[...] = eliminate(state_ref[...], start, stop)

        @scoped
        def project():
            @apart
            def _():
                proj[pl.ds(0, rows), :] = projector_end(state_ref[...], weight_ref, obs_ref)

            z_copy(TILES).start()
            x_copy(TILES).start()
            share(0, TILES).start()

        def gather_sent():
            for slot in range(TILES + 1):
                when(to_z_peer(slot), lambda: z_copy(slot).wait_send())
                when(at_x_peer(slot), lambda: x_copy(slot).wait_send())
                when(at_x_peer(slot), lambda: relay(slot).wait_send())
                for chip in range(4):
                    when(here(slot), lambda: share(chip, slot).wait_send())

        def sum_sent(n):
            for copy in straight(n) if n in straight_jobs else [stage_one(n, 0), stage_one(n, 1), stage_two(n)]:
                copy.wait_send()

        def right_side_row():
            turned_rows = proj[...].astype(jnp.float32).T.astype(jnp.bfloat16)
            right_lhs[...] = turned_rows[rows : rows + 16]

        def add_vectors():
            total = vec[2 * near + y, :1, :]
            for k in range(3):
                vector_copy(k).wait_recv()
                total = total + vec_in[k, :1, :]
            right_ref[...] = total[:, : 2 * rows]
            tail_ref[...] = total[:, 2 * rows : 3 * rows]


        if side == 0:
            start_share(3)
            start_share(1)
            start_x(1)
            start_z(1)
            sweep(0 * rows // 80, 16 * rows // 80)
            start_x(2)
            sweep(16 * rows // 80, 32 * rows // 80)
            start_share(4)
            sweep(32 * rows // 80, 48 * rows // 80)
            start_z(0)
            start_share(6)
            sweep(48 * rows // 80, 64 * rows // 80)
            sweep(64 * rows // 80, 80 * rows // 80)
            from_z(1)
            from_x(0)
            start_share(0)
            start_share(5)
            start_x(3)
            z_mid(2)
            z_end(2)
            start_share(2)
            start_x(4)
            project()
            z_mid(3)
            start_x(0)
            from_z(TILES)
            from_z(0)
            z_mid(4)
            from_x(2)
            from_relay(0)
            z_end(3)
            from_z(2)
            from_x(1)
            from_x(TILES)
            z_mid(5)
            z_end(4)
            start_share(7)
            from_relay(TILES)
            settled(0)
            from_relay(1)
            settled(TILES)
            from_x(4)
            settled(1)
            make_lhs(0)
            jobs_at(1)
            from_z(3)
            from_relay(2)
            right_side_row()
            start_x(6)
            z_end(5)
            start_x(7)
            start_x(5)
            z_mid(6)
            settled(2)
            jobs_at(2)
            from_z(4)
            z_end(7)
            from_relay(3)
            z_mid(7)
            from_x(3)
            z_end(6)
            settled(3)
            from_z(5)
            jobs_at(3)
            pass_on(0)
            from_relay(4)
            from_x(6)
            settled(4)
            jobs_at(4)
            pass_on(2)
            from_x(5)
            from_relay(5)
            settled(5)
            from_z(6)
            from_z(7)
            jobs_at(5)
            from_relay(6)
            from_x(7)
            pass_on(1)
            pass_on(3)
            finish(0)
            from_relay(7)
            settled(6)
            jobs_at(6)
            finish(2)
            pass_on(4)
            settled(7)
            jobs_at(7)
            vectors()
            pass_on(5)
            pass_on(6)
            finish(1)
            pass_on(7)
            finish(4)
            finish(3)
            gather_sent()
            sum_sent(0)
            sum_sent(2)
            sum_sent(1)
            sum_sent(4)
            sum_sent(3)
            finish(6)
            finish(5)
            add_vectors()
            finish(7)
            sum_sent(6)
            sum_sent(5)
            sum_sent(7)
            for k in range(3):
                vector_copy(k).wait_send()
        else:
            start_z(0)
            from_x(0)
            start_share(0)
            start_share(3)
            sweep(0 * rows // 80, 16 * rows // 80)
            start_x(0)
            sweep(16 * rows // 80, 32 * rows // 80)
            start_z(1)
            sweep(32 * rows // 80, 48 * rows // 80)
            start_x(2)
            start_share(7)
            start_share(2)
            sweep(48 * rows // 80, 64 * rows // 80)
            start_share(5)
            start_x(1)
            sweep(64 * rows // 80, 80 * rows // 80)
            project()
            start_share(1)
            from_z(0)
            z_mid(2)
            from_z(TILES)
            z_mid(3)
            from_z(1)
            from_relay(1)
            from_x(1)
            z_mid(6)
            from_relay(0)
            z_mid(4)
            z_end(2)
            start_share(6)
            settled(0)
            start_x(4)
            z_end(3)
            start_share(4)
            from_x(2)
            z_end(4)
            start_x(3)
            settled(1)
            from_z(2)
            from_x(TILES)
            from_relay(TILES)
            settled(TILES)
            from_relay(2)
            make_lhs(0)
            settled(2)
            from_z(3)
            from_x(3)
            z_end(5)
            jobs_at(1)
            jobs_at(2)
            start_x(6)
            start_x(5)
            from_relay(3)
            settled(3)
            z_mid(5)
            jobs_at(3)
            from_x(4)
            z_mid(7)
            right_side_row()
            pass_on(0)
            from_z(4)
            z_end(6)
            from_x(6)
            from_relay(4)
            from_z(5)
            settled(4)
            settled(7)
            z_end(7)
            jobs_at(4)
            from_relay(5)
            start_x(7)
            from_x(5)
            pass_on(2)
            pass_on(3)
            settled(5)
            pass_on(1)
            from_z(6)
            jobs_at(5)
            from_z(7)
            from_relay(6)
            settled(6)
            pass_on(4)
            pass_on(5)
            jobs_at(6)
            vectors()
            finish(3)
            finish(0)
            pass_on(6)
            pass_on(7)
            finish(4)
            finish(7)
            finish(1)
            from_x(7)
            gather_sent()
            sum_sent(3)
            sum_sent(0)
            sum_sent(4)
            sum_sent(7)
            sum_sent(1)
            finish(6)
            jobs_at(7)
            finish(2)
            from_relay(7)
            add_vectors()
            finish(5)
            sum_sent(6)
            sum_sent(2)
            sum_sent(5)
            for k in range(3):
                vector_copy(k).wait_send()

    @pl.when(mission == 0)
    def _():
        run(0)

    @pl.when(mission == 1)
    def _():
        run(1)

def on_paired_chips(
    design,
    nuisance_design,
    observed,
    arc_of_row,
    nuis_size,
    weight_index,
    kind_weight,
    mission_weight,
):
    rows, width_all = design.shape
    wide = rounded_up(rows + 1, LANES)
    tile_cols = width_all // TILES
    stacked = 2 * 4 * rows
    vec_cols = rounded_up(3 * rows, LANES)
    vmem = pl.BlockSpec(memory_space=pltpu.VMEM)
    smem = pl.BlockSpec(memory_space=pltpu.SMEM)
    dma = pltpu.SemaphoreType.DMA
    slots = TILES + 1

    fold, right, tail = pl.pallas_call(
        normals_kernel,
        out_shape=(
            pltpu.VMEM((rows, width_all), jnp.float32),
            pltpu.VMEM((1, 2 * rows), jnp.float32),
            pltpu.VMEM((1, rows), jnp.float32),
        ),
        in_specs=[smem, smem, vmem, pl.BlockSpec(memory_space=pl.ANY), vmem, vmem, vmem, vmem],
        out_specs=(vmem, vmem, vmem),
        scratch_shapes=[
            pltpu.VMEM((TILES, stacked, tile_cols), jnp.bfloat16),
            pltpu.VMEM((stacked, wide), jnp.bfloat16),
            pltpu.VMEM((rows, wide), jnp.float32),
            pltpu.VMEM((tile_cols, stacked), jnp.bfloat16),
            pltpu.VMEM((2, 4 * rows, stacked), jnp.bfloat16),
            pltpu.VMEM((16, stacked), jnp.bfloat16),
            pltpu.VMEM((TILES, 2, 2, rows, tile_cols), jnp.bfloat16),
            pltpu.VMEM((TILES, 2, rows, tile_cols), jnp.bfloat16),
            pltpu.VMEM((TILES, rows, tile_cols), jnp.bfloat16),
            pltpu.VMEM((TILES, rows, tile_cols), jnp.bfloat16),
            pltpu.VMEM((4, 8, vec_cols), jnp.float32),
            pltpu.VMEM((3, 8, vec_cols), jnp.float32),
            dma((TILES,)),
            dma((slots,)),
            dma((slots,)),
            dma((slots,)),
            dma((slots,)),
            dma((slots,)),
            dma((slots,)),
            dma((4, slots)),
            dma((4, slots)),
            dma((TILES, 2)),
            dma((TILES, 2)),
            dma((TILES,)),
            dma((TILES,)),
            dma((1, 3)),
            dma((1, 3)),
            dma((3,)),
            dma((3,)),
        ],
        compiler_params=pltpu.CompilerParams(
            collective_id=0, has_side_effects=True, vmem_limit_bytes=60 * 2**20
        ),
        name="normals",
    )(
        nuis_size,
        kind_weight,
        mission_weight,
        design,
        nuisance_design,
        arc_of_row,
        weight_index,
        observed,
    )
    return fold, right.reshape(-1), tail.reshape(-1)


def solution(mesh):
    placed = (
        P(("mission", "arc"), None),
        P(("mission", "arc"), None),
        P(("mission", "arc")),
        P(("mission", "arc")),
        P(("mission", "arc")),
        P(("mission", "arc")),
        P(),
        P("mission"),
    )

    def on_device(design, *rest):
        devices = lax.axis_size("mission") * lax.axis_size("arc")
        paired = lax.axis_size("mission") == 2 and lax.axis_size("arc") == 16
        rows, width_all = design.shape
        if paired and width_all == 2 * devices * rows and rows % 16 == 0 and width_all % (TILES * LANES) == 0:
            return on_paired_chips(design, *rest)
        return on_any_mesh(design, *rest)

    return jax.shard_map(
        on_device,
        mesh=mesh,
        in_specs=placed,
        out_specs=(P(("mission", "arc"), None), P(("mission", "arc")), P(("mission", "arc"))),
        check_vma=False,
    )
```
